256 devices in a mesh: tm: 32 (over z, x), strip: 8 (over y, core).
Axes of the slice: x: 4, y: 4, z: 8, core: 2. Of those that a mesh axis runs over, the one named last changes fastest.
Arguments:
- coarse_feat: bfloat16 [128, 96, 4, 384], P('tm', 'strip'), may hold values from -6 to 6
- coarse_gain: float32 [384], replicated, may hold values from 0.5 to 2
- coarse_weight: bfloat16 [3, 3, 3, 384, 384], replicated, may hold values from -0.0625 to 0.0625
- coarse_bias: float32 [384], replicated, may hold values from -3 to 3
- up_weight: bfloat16 [3, 3, 384, 192], replicated, may hold values from -0.109375 to 0.109375
- up_bias: float32 [192], replicated, may hold values from -3 to 3
- fine_gain: float32 [192], replicated, may hold values from 0.5 to 2
- fine_weight: bfloat16 [3, 3, 3, 192, 192], replicated, may hold values from -0.078125 to 0.078125
- fine_bias: float32 [192], replicated, may hold values from -3 to 3
Outputs:
- decoded: bfloat16 [128, 192, 8, 192], P('tm', 'strip')
The draws below stay inside these ranges and needn't reach their ends.
All inputs are finite; a program needn't handle non-finite values.
Results may differ from the reference program's by a relative error of at most 0.0095.
Values may be sent and summed in bfloat16 or wider, within the bound.
No kernel may reach another device: no remote copies, remote signals or barrier semaphores. Data moves between devices by JAX's collectives and lax.ppermute only.
A program may use at most 64 MiB of HBM per device.

```python
import math
import jax
import jax.numpy as jnp
from jax import lax

C0 = 384
C1 = 192
WW = 4
FRAMES = 128
ROWS = 96


def steps_of(key, extent, split, low, top_value):
    def one(axis_at, parts):
        draws = jax.random.uniform(jax.random.fold_in(jax.random.fold_in(key, 6), axis_at), (parts,), jnp.float32, low / len(split), top_value / len(split))
        return jnp.repeat(jnp.exp(draws), extent[axis_at] // parts).reshape((-1,) + (1,) * (len(extent) - axis_at - 1))

    level = one(*split[0])
    for cut in split[1:]:
        level = level * one(*cut)
    return level


def gaussian(own_key, extent, width, limit, cuts=(), held_as=jnp.bfloat16):
    entries = jax.random.normal(own_key, extent, jnp.float32) * width
    if len(cuts) > 0:
        entries = steps_of(own_key, extent, cuts, -0.22, 0.18) * entries
    return jnp.clip(entries, min=-limit, max=limit).astype(held_as)


def setup_inputs(seed: int = 0) -> dict:
    keys = jax.random.split(jax.random.key(seed), 10)
    coarse_feat = gaussian(keys[0], (FRAMES, ROWS, WW, C0), 1.0, 6.0, ((0, 32), (1, 8)))
    coarse_gain = jnp.clip(jnp.exp(jax.random.uniform(keys[1], (C0,), jnp.float32, math.log(0.5), math.log(2.0))), 0.5, 2.0)
    coarse_weight = gaussian(keys[2], (3, 3, 3, C0, C0), (27 * C0) ** -0.5, 0.0625)
    coarse_bias = gaussian(keys[3], (C0,), 0.5, 3.0, (), jnp.float32)
    up_weight = gaussian(keys[4], (3, 3, C0, C1), (9 * C0) ** -0.5, 0.109375)
    up_bias = gaussian(keys[5], (C1,), 0.5, 3.0, (), jnp.float32)
    fine_gain = jnp.clip(jnp.exp(jax.random.uniform(keys[6], (C1,), jnp.float32, math.log(0.5), math.log(2.0))), 0.5, 2.0)
    fine_weight = gaussian(keys[7], (3, 3, 3, C1, C1), (27 * C1) ** -0.5, 0.078125)
    fine_bias = gaussian(keys[8], (C1,), 0.5, 3.0, (), jnp.float32)
    return dict(coarse_feat=coarse_feat, coarse_gain=coarse_gain, coarse_weight=coarse_weight, coarse_bias=coarse_bias, up_weight=up_weight, up_bias=up_bias, fine_gain=fine_gain, fine_weight=fine_weight, fine_bias=fine_bias)


eps = 1e-06

def prep(feat, gain):
    values = feat.astype(jnp.float32)
    meansq = lax.optimization_barrier(jnp.mean(values * values, axis=-1, keepdims=True))
    return jax.nn.silu(values * lax.rsqrt(meansq + eps) * gain).astype(jnp.bfloat16)

def causal_conv(act, kernel):
    out = lax.conv_general_dilated(act.astype(jnp.float32)[None], kernel.astype(jnp.float32), (1, 1, 1), [(2, 0), (1, 1), (1, 1)], dimension_numbers=('NDHWC', 'DHWIO', 'NDHWC'))
    return out[0]

def plane_conv(act, kernel):
    return lax.conv_general_dilated(act.astype(jnp.float32), kernel.astype(jnp.float32), (1, 1), [(1, 1), (1, 1)], dimension_numbers=('NHWC', 'HWIO', 'NHWC'))

def reference(coarse_feat, coarse_gain, coarse_weight, coarse_bias, up_weight, up_bias, fine_gain, fine_weight, fine_bias):
    act0 = prep(coarse_feat, coarse_gain)
    coarse = (causal_conv(act0, coarse_weight) + coarse_bias).astype(jnp.bfloat16)
    upper = jnp.repeat(jnp.repeat(coarse, 2, axis=1), 2, axis=2)
    lifted = (plane_conv(upper, up_weight) + up_bias).astype(jnp.bfloat16)
    act1 = prep(lifted, fine_gain)
    decoded = causal_conv(act1, fine_weight) + fine_bias + lifted.astype(jnp.float32)
    return decoded.astype(jnp.bfloat16)
```

```python
import functools

import jax
import jax.numpy as jnp
from jax import lax
from jax.experimental import pallas as pl
from jax.experimental.pallas import tpu as pltpu
from jax.sharding import PartitionSpec as P

EPS = 1e-6
BF = jnp.bfloat16
F32 = jnp.float32


def silu(v):
    half = 0.5 * v
    return half + half * jnp.tanh(half)


def dot(a, b):
    return jnp.dot(a, b, preferred_element_type=F32)


def kernel(last, x, prev, above, below, gain0, wc, bias0, w4, bias1, gain1, wf, bias2, out,
           raw, left, mid, lift, planes, nat, back):
    group = lax.axis_index("tm")
    strip = lax.axis_index("strip")
    c0 = wc.shape[-1]
    c1 = wf.shape[-1]
    for t in range(8):
        src, f = (prev, t) if t < 4 else (x, t - 4)
        base = 64 * t
        for h in range(16):
            v = above[t, h] if h < 2 else below[t, h - 14] if h > 13 else src[f, h - 2]
            for c in range(3):
                raw[c, base + 4 * h:base + 4 * h + 4, :] = v[:, 128 * c:128 * c + 128].astype(F32)
    g0 = gain0[...]
    for t in range(8):
        v = jnp.concatenate([raw[c, 64 * t:64 * t + 64, :] for c in range(3)], axis=1)
        r = lax.rsqrt(jnp.mean(v * v, axis=-1, keepdims=True) + EPS)
        v = silu(v * r * g0)
        for c in range(3):
            raw[c, 64 * t:64 * t + 64, :] = v[:, 128 * c:128 * c + 128]
    for kh in range(3):
        for t in range(8):
            for w in range(4):
                for c in range(3):
                    v = raw[c, pl.ds(64 * t + 4 * kh + w, 16, stride=4), :]
                    left[kh, 64 * t + 16 * w:64 * t + 16 * w + 16, 128 * c:128 * c + 128] = v.astype(BF)

    def taps(kw, lo, n):
        cols = []
        for kt in range(3):
            for kh in range(3):
                cols.append(jnp.concatenate(
                    [left[kh, 64 * (t + kt) + 16 * lo:64 * (t + kt) + 16 * (lo + n), :] for t in range(6)], axis=0))
        lhs = jnp.concatenate(cols, axis=1)
        rhs = jnp.concatenate([wc[kt, kh, kw] for kt in range(3) for kh in range(3)], axis=0)
        return dot(lhs, rhs)

    b0 = bias0[...]
    mid[0:384, :] = taps(1, 0, 4) + b0
    p = taps(0, 0, 3)
    for t in range(6):
        mid[64 * t + 16:64 * t + 64, :] += p[48 * t:48 * t + 48]
    p = taps(2, 1, 3)
    for t in range(6):
        mid[64 * t:64 * t + 48, :] += p[48 * t:48 * t + 48]
    row = lax.broadcasted_iota(jnp.int32, (16, c0), 0)
    keep = jnp.logical_and(jnp.logical_or(strip > 0, row != 0), jnp.logical_or(strip < last, row != 13))
    for t in range(6):
        for w in range(4):
            at = 64 * t + 16 * w
            v = jnp.where(keep, mid[at:at + 16, :], 0.0)
            mid[at:at + 16, :] = v
    for t in range(6):
        for w in range(4):
            at = 64 * t + 16 * w
            left[0, at:at + 16, :] = mid[at:at + 16, :].astype(BF)
            left[1, at:at + 16, :] = mid[at + 1:at + 17, :].astype(BF)

    def ups(lo, n):
        a = jnp.concatenate([left[0, 64 * t + 16 * lo:64 * t + 16 * (lo + n), :] for t in range(6)], axis=0)
        b = jnp.concatenate([left[1, 64 * t + 16 * lo:64 * t + 16 * (lo + n), :] for t in range(6)], axis=0)
        return jnp.concatenate([a, b], axis=1)

    b1 = bias1[...]
    b1 = jnp.concatenate([b1, b1], axis=1)
    g1 = gain1[...]
    g1 = jnp.concatenate([g1, g1], axis=1)
    lane = lax.broadcasted_iota(jnp.int32, (16, 2 * c1), 1)
    even = lane < c1
    row = lax.broadcasted_iota(jnp.int32, (16, 2 * c1), 0)

    def finish(u, p, t, a):
        l = (u + b1).astype(BF).astype(F32)
        lift[a, p, 16 * t:16 * t + 16, :] = l
        sq = l * l
        me = jnp.sum(jnp.where(even, sq, 0.0), axis=-1, keepdims=True) * (1.0 / c1)
        mo = jnp.sum(jnp.where(even, 0.0, sq), axis=-1, keepdims=True) * (1.0 / c1)
        r = jnp.where(even, lax.rsqrt(me + EPS), lax.rsqrt(mo + EPS))
        v = silu(l * r * g1)
        if p == 0:
            v = jnp.where(even, v, 0.0)
        if p == 4:
            v = jnp.where(even, 0.0, v)
        if a == 0:
            ok = jnp.logical_or(strip < last, row != 12)
        else:
            ok = jnp.logical_or(strip > 0, row != 0)
        if t < 2:
            ok = jnp.logical_and(ok, group > 0)
        nat[a, 0:16, 0:2 * c1] = jnp.where(ok, v, 0.0)
        planes[a, 0, p, 16 * t:16 * t + 16, :] = nat[a, 0:16, 0:2 * c1].astype(BF)
        planes[a, 1, p, 16 * t:16 * t + 16, :] = nat[a, 1:17, 0:2 * c1].astype(BF)

    u = dot(jnp.concatenate([ups(0, 3), ups(1, 3)], axis=1), w4[...])
    for t in range(6):
        for p in range(1, 4):
            for a in range(2):
                finish(u[48 * t + 16 * p - 16:48 * t + 16 * p, 2 * c1 * a:2 * c1 * (a + 1)], p, t, a)
    u = dot(ups(0, 1), w4[2 * c0:, :])
    for t in range(6):
        for a in range(2):
            finish(u[16 * t:16 * t + 16, 2 * c1 * a:2 * c1 * (a + 1)], 0, t, a)
    u = dot(ups(3, 1), w4[:2 * c0, :])
    for t in range(6):
        for a in range(2):
            finish(u[16 * t:16 * t + 16, 2 * c1 * a:2 * c1 * (a + 1)], 4, t, a)

    b2 = bias2[...]
    zero = jnp.zeros((64, c1), BF)
    for a in range(2):
        reads = ((1, 0), (0, 0), (1, 1)) if a == 0 else ((0, 0), (1, 1), (0, 1))
        for b in range(2):
            cols, rhs = [], []
            for kt in range(3):
                for kh in range(3):
                    ph, sh = reads[kh]
                    first = jnp.concatenate([planes[ph, sh, q, 16 * kt:16 * kt + 64, :] for q in range(4)], axis=0)
                    second = jnp.concatenate([planes[ph, sh, q + 1, 16 * kt:16 * kt + 64, :] for q in range(4)], axis=0)
                    k0, k1, k2 = (wf[kt, kh, kw] for kw in range(3))
                    if b == 0:
                        cols += [first, second[:, 128:]]
                        rhs += [k1, k0, zero, k2]
                    else:
                        cols += [first[:, :256], second]
                        rhs += [k0, zero, k2, k1]
            d = dot(jnp.concatenate(cols, axis=1), jnp.concatenate(rhs, axis=0)) + b2
            for q in range(4):
                for t in range(4):
                    p = q if b == 0 else q + 1
                    at = 16 * (t + 2) + a
                    l = lift[a, p, at:at + 12, :]
                    l = l[:, :c1] if b == 0 else l[:, c1:]
                    v = d[64 * q + 16 * t:64 * q + 16 * t + 12, :] + l
                    nat_rows = pl.ds((24 * t + a) * 8 + 2 * q + b, 12, stride=16)
                    back[0, nat_rows, :] = v[:, :128]
                    back[1, nat_rows, 0:64] = v[:, 128:]
    for t in range(4):
        v = jnp.concatenate([back[0, 192 * t:192 * t + 192, :], back[1, 192 * t:192 * t + 192, 0:64]], axis=1)
        out[t] = v.reshape(24, 8, c1).astype(BF)


def block(x, gain0, wc, bias0, wu, bias1, gain1, wf, bias2, *, nt, ns):
    c0, c1 = wc.shape[-1], wf.shape[-1]
    at = lambda t, s: t * ns + s
    axes = ("tm", "strip")
    prev = lax.ppermute(x, axes, [(at(t, s), at(t + 1, s)) for t in range(nt - 1) for s in range(ns)])
    both = jnp.concatenate([prev, x], axis=0)
    above = lax.ppermute(both[:, 10:], axes, [(at(t, s), at(t, s + 1)) for t in range(nt) for s in range(ns - 1)])
    below = lax.ppermute(both[:, :2], axes, [(at(t, s + 1), at(t, s)) for t in range(nt) for s in range(ns - 1)])
    f = wu.astype(F32)
    first, second = ((0,), (1, 2)), ((0, 1), (2,))
    pick = (first, second)
    rows = []
    for wcol in range(2):
        for hrow in range(2):
            rows.append(jnp.concatenate(
                [sum(f[kh, kw] for kh in pick[a][hrow] for kw in pick[b][wcol]) for a in range(2) for b in range(2)],
                axis=1))
    w4 = jnp.concatenate(rows, axis=0).astype(BF)
    vm = pl.BlockSpec(memory_space=pltpu.VMEM)
    two = lambda v: v.reshape(1, -1)
    return pl.pallas_call(
        functools.partial(kernel, ns - 1),
        out_shape=jax.ShapeDtypeStruct((4, 24, 8, c1), BF),
        in_specs=[vm] * 12,
        out_specs=vm,
        scratch_shapes=[
            pltpu.VMEM((3, 528, 128), F32),
            pltpu.VMEM((3, 512, c0), BF),
            pltpu.VMEM((400, c0), F32),
            pltpu.VMEM((2, 5, 112, 2 * c1), F32),
            pltpu.VMEM((2, 2, 5, 96, 2 * c1), BF),
            pltpu.VMEM((2, 32, 2 * c1), F32),
            pltpu.VMEM((2, 768, 128), F32),
        ],
        compiler_params=pltpu.CompilerParams(vmem_limit_bytes=40 << 20),
    )(x, prev, above, below, two(gain0), wc, two(bias0), w4, jnp.concatenate([two(bias1)], axis=1), two(gain1), wf, two(bias2))


def solution(mesh):
    nt, ns = mesh.shape["tm"], mesh.shape["strip"]
    part = P("tm", "strip", None, None)
    return jax.shard_map(
        functools.partial(block, nt=nt, ns=ns), mesh=mesh,
        in_specs=(part,) + (P(),) * 8, out_specs=part, check_vma=False)
```

```python
import functools

import jax
import jax.numpy as jnp
from jax import lax
from jax.experimental import pallas as pl
from jax.experimental.pallas import tpu as pltpu
from jax.sharding import PartitionSpec as P


EPS = 1e-6
BF = jnp.bfloat16
F32 = jnp.float32


def silu(v):
    half = 0.5 * v
    return half + half * jnp.tanh(half)


def dot(a, b):
    return jnp.dot(a, b, preferred_element_type=F32)


def phases(wu, w4, turned):
    c1, c0 = wu.shape[2:]
    for r in range(0, c1, 16):
        f = [[wu[kh, kw, r:r + 16, :].astype(F32) for kw in range(3)] for kh in range(3)]
        cols = [[(k[0], k[1] + k[2]), (k[0] + k[1], k[2])] for k in f]
        for wcol in range(2):
            tap = [[cols[kh][b][wcol] for b in range(2)] for kh in range(3)]
            first = tap[0] + [tap[0][b] + tap[1][b] for b in range(2)]
            second = [tap[1][b] + tap[2][b] for b in range(2)] + tap[2]
            for hrow, parts in enumerate((first, second)):
                at = (2 * wcol + hrow) * c0
                for i, v in enumerate(parts):
                    turned[c1 * i + r:c1 * i + r + 16, at:at + c0] = v.astype(BF)
    for k in range(0, 4 * c0, 128):
        w4[k:k + 128, :] = turned[:, k:k + 128].T


def put(raw, row, v):
    for c in range(3):
        raw[c, row:row + v.shape[0], :] = v[:, 128 * c:128 * c + 128]


def normed(raw, row, g0):
    v = jnp.concatenate([raw[c, row:row + 64, :] for c in range(3)], axis=1)
    r = lax.rsqrt(jnp.mean(v * v, axis=-1, keepdims=True) + EPS)
    return silu(v * r * g0)


def spread(raw, left, t):
    for kh in range(3):
        for w in range(4):
            for c in range(3):
                v = raw[c, pl.ds(64 * t + 4 * kh + w, 16, stride=4), :]
                left[kh, 64 * t + 16 * w:64 * t + 16 * w + 16, 128 * c:128 * c + 128] = v.astype(BF)


SPAN = ((0, 3), (0, 4), (1, 3))


def own(x, gain0, wc, wu, w4, wv, part, turned, raw, left, sems):
    copies = {}
    for kt in (2, 1, 0):
        copies[kt] = pltpu.make_async_copy(wc.at[kt], wv.at[kt], sems.at[kt])
        copies[kt].start()
    phases(wu, w4, turned)
    g0 = gain0[...]
    zero = jnp.zeros((8, x.shape[-1]), F32)
    for t in range(4):
        put(raw, 64 * t, zero)
        put(raw, 64 * t + 56, zero)
        for h in range(12):
            put(raw, 64 * t + 8 + 4 * h, x[t, h].astype(F32))
    put(raw, 256, zero)
    for t in range(4):
        put(raw, 64 * t, normed(raw, 64 * t, g0))
    for t in range(4):
        spread(raw, left, t)
    for kt in (2, 1, 0):
        copies[kt].wait()
        n = kt + 2
        for kw in (1, 0, 2):
            lo, m = SPAN[kw]
            lhs = jnp.concatenate(
                [jnp.concatenate([left[kh, 64 * t + 16 * lo:64 * t + 16 * (lo + m), :] for t in range(n)], axis=0)
                 for kh in range(3)], axis=1)
            d = dot(lhs, jnp.concatenate([wv[kt, kh, kw] for kh in range(3)], axis=0))
            for t in range(n):
                at = 64 * (t + 2 - kt) + 16 * (lo + 1 - kw)
                v = d[16 * m * t:16 * m * (t + 1)]
                if kt == 2 and kw == 1:
                    part[at:at + 16 * m, :] = v
                else:
                    part[at:at + 16 * m, :] += v


def kernel(last, part, prev, outer, inner, gain0, wc, bias0, w4, bias1, gain1, wf, bias2, out,
           raw, left, ends, tail, mid, lift, planes, nat, back):
    group = lax.axis_index("tm")
    strip = lax.axis_index("strip")
    c0 = wc.shape[-1]
    c1 = wf.shape[-1]
    odd = strip % 2 == 1

    def margin(t, h):
        i, o = inner[t, h % 2].astype(F32), outer[t, h % 2].astype(F32)
        return jnp.where(odd, i, o) if h < 2 else jnp.where(odd, o, i)

    for t in range(4):
        for h in range(16):
            put(raw, 64 * t + 4 * h, prev[t, h - 2].astype(F32) if 1 < h < 14 else margin(t, h))
        for i, h in enumerate((0, 1, 14, 15)):
            put(raw, 256 + 16 * t + 4 * i, margin(4 + t, h))
    g0 = gain0[...]
    for t in range(4):
        put(raw, 64 * t, normed(raw, 64 * t, g0))
    v = normed(raw, 256, g0)
    row = lax.broadcasted_iota(jnp.int32, (8, c0), 0)
    none = jnp.zeros((8, c0), F32)
    for t in range(4):
        up, down = v[16 * t:16 * t + 8], v[16 * t + 8:16 * t + 16]
        for kh in range(3):
            a = (up, jnp.where(row < 4, pltpu.roll(up, 4, 0), 0.0), none)[kh]
            b = (none, jnp.where(row < 4, 0.0, pltpu.roll(down, 4, 0)), down)[kh]
            for kw in range(3):
                if kw == 0:
                    e = [jnp.where(row % 4 == 0, 0.0, pltpu.roll(z, 1, 0)) for z in (a, b)]
                elif kw == 2:
                    e = [jnp.where(row % 4 == 3, 0.0, pltpu.roll(z, 7, 0)) for z in (a, b)]
                else:
                    e = [a, b]
                ends[kw, kh, 16 * t:16 * t + 16, :] = jnp.concatenate(e, axis=0).astype(BF)
    for t in range(4):
        spread(raw, left, t)

    b0 = bias0[...]
    for t in range(2):
        mid[64 * t:64 * t + 64, :] = jnp.broadcast_to(b0, (64, c0))
    mid[128:384, :] = part[...] + b0
    for kt in range(3):
        n = 4 - kt
        for kw in range(3):
            lo, m = SPAN[kw]
            lhs = jnp.concatenate(
                [jnp.concatenate(
                    [left[kh, 64 * (u + kt) + 16 * lo:64 * (u + kt) + 16 * (lo + m), :] for u in range(n)]
                    + [ends[kw, kh, 0:16 * (kt + 2), :]], axis=0)
                 for kh in range(3)], axis=1)
            d = dot(lhs, jnp.concatenate([wc[kt, kh, kw] for kh in range(3)], axis=0))
            for u in range(n):
                at = 64 * u + 16 * (lo + 1 - kw)
                mid[at:at + 16 * m, :] += d[16 * m * u:16 * m * (u + 1)]
            for i in range(kt + 2):
                e = d[16 * (m * n + i):16 * (m * n + i + 1)]
                at = 16 * (i + 2 - kt)
                for c in range(3):
                    if kt == 0 and kw == 0:
                        tail[c, at:at + 16, :] = e[:, 128 * c:128 * c + 128]
                    else:
                        new = kw == 0 and i == 0
                        old = 0.0 if new else tail[c, at:at + 16, :]
                        tail[c, at:at + 16, :] = old + e[:, 128 * c:128 * c + 128]
    for t in range(4):
        for w in range(4):
            for c in range(3):
                for i, r in enumerate((0, 12)):
                    at = 64 * (t + 2) + 16 * w + r
                    mid[at:at + 2, 128 * c:128 * c + 128] += tail[c, pl.ds(16 * t + 8 * i + w, 2, stride=4), :]
    row = lax.broadcasted_iota(jnp.int32, (16, c0), 0)
    keep = jnp.logical_and(jnp.logical_or(strip > 0, row != 0), jnp.logical_or(strip < last, row != 13))
    for t in range(6):
        for w in range(4):
            at = 64 * t + 16 * w
            v = jnp.where(keep, mid[at:at + 16, :], 0.0)
            mid[at:at + 16, :] = v
    for t in range(6):
        for w in range(4):
            at = 64 * t + 16 * w
            left[0, at:at + 16, :] = mid[at:at + 16, :].astype(BF)
            left[1, at:at + 16, :] = mid[at + 1:at + 17, :].astype(BF)

    def ups(lo, n):
        a = jnp.concatenate([left[0, 64 * t + 16 * lo:64 * t + 16 * (lo + n), :] for t in range(6)], axis=0)
        b = jnp.concatenate([left[1, 64 * t + 16 * lo:64 * t + 16 * (lo + n), :] for t in range(6)], axis=0)
        return jnp.concatenate([a, b], axis=1)

    b1 = bias1[...]
    b1 = jnp.concatenate([b1, b1], axis=1)
    g1 = gain1[...]
    g1 = jnp.concatenate([g1, g1], axis=1)
    lane = lax.broadcasted_iota(jnp.int32, (16, 2 * c1), 1)
    even = lane < c1
    row = lax.broadcasted_iota(jnp.int32, (16, 2 * c1), 0)

    def finish(u, p, t, a):
        l = (u + b1).astype(BF).astype(F32)
        lift[a, p, 16 * t:16 * t + 16, :] = l
        sq = l * l
        me = jnp.sum(jnp.where(even, sq, 0.0), axis=-1, keepdims=True) * (1.0 / c1)
        mo = jnp.sum(jnp.where(even, 0.0, sq), axis=-1, keepdims=True) * (1.0 / c1)
        r = jnp.where(even, lax.rsqrt(me + EPS), lax.rsqrt(mo + EPS))
        v = silu(l * r * g1)
        if p == 0:
            v = jnp.where(even, v, 0.0)
        if p == 4:
            v = jnp.where(even, 0.0, v)
        if a == 0:
            ok = jnp.logical_or(strip < last, row != 12)
        else:
            ok = jnp.logical_or(strip > 0, row != 0)
        if t < 2:
            ok = jnp.logical_and(ok, group > 0)
        nat[a, 0:16, 0:2 * c1] = jnp.where(ok, v, 0.0)
        planes[a, 0, p, 16 * t:16 * t + 16, :] = nat[a, 0:16, 0:2 * c1].astype(BF)
        planes[a, 1, p, 16 * t:16 * t + 16, :] = nat[a, 1:17, 0:2 * c1].astype(BF)

    u = dot(jnp.concatenate([ups(0, 3), ups(1, 3)], axis=1), w4[...])
    for t in range(6):
        for p in range(1, 4):
            for a in range(2):
                finish(u[48 * t + 16 * p - 16:48 * t + 16 * p, 2 * c1 * a:2 * c1 * (a + 1)], p, t, a)
    u = dot(ups(0, 1), w4[2 * c0:, :])
    for t in range(6):
        for a in range(2):
            finish(u[16 * t:16 * t + 16, 2 * c1 * a:2 * c1 * (a + 1)], 0, t, a)
    u = dot(ups(3, 1), w4[:2 * c0, :])
    for t in range(6):
        for a in range(2):
            finish(u[16 * t:16 * t + 16, 2 * c1 * a:2 * c1 * (a + 1)], 4, t, a)

    b2 = bias2[...]
    zero = jnp.zeros((64, c1), BF)
    for a in range(2):
        reads = ((1, 0), (0, 0), (1, 1)) if a == 0 else ((0, 0), (1, 1), (0, 1))
        for b in range(2):
            cols, rhs = [], []
            for kt in range(3):
                for kh in range(3):
                    ph, sh = reads[kh]
                    first = jnp.concatenate([planes[ph, sh, q, 16 * kt:16 * kt + 64, :] for q in range(4)], axis=0)
                    second = jnp.concatenate([planes[ph, sh, q + 1, 16 * kt:16 * kt + 64, :] for q in range(4)], axis=0)
                    k0, k1, k2 = (wf[kt, kh, kw] for kw in range(3))
                    if b == 0:
                        cols += [first, second[:, 128:]]
                        rhs += [k1, k0, zero, k2]
                    else:
                        cols += [first[:, :256], second]
                        rhs += [k0, zero, k2, k1]
            d = dot(jnp.concatenate(cols, axis=1), jnp.concatenate(rhs, axis=0)) + b2
            for q in range(4):
                for t in range(4):
                    p = q if b == 0 else q + 1
                    at = 16 * (t + 2) + a
                    l = lift[a, p, at:at + 12, :]
                    l = l[:, :c1] if b == 0 else l[:, c1:]
                    v = d[64 * q + 16 * t:64 * q + 16 * t + 12, :] + l
                    nat_rows = pl.ds((24 * t + a) * 8 + 2 * q + b, 12, stride=16)
                    back[0, nat_rows, :] = v[:, :128]
                    back[1, nat_rows, 0:64] = v[:, 128:]
    for t in range(4):
        v = jnp.concatenate([back[0, 192 * t:192 * t + 192, :], back[1, 192 * t:192 * t + 192, 0:64]], axis=1)
        out[t] = v.reshape(24, 8, c1).astype(BF)


def block(x, gain0, wc, bias0, wu, bias1, gain1, wf, bias2, *, nt, ns):
    c0, c1 = wc.shape[-1], wf.shape[-1]
    at = lambda t, s: t * ns + s
    axes = ("tm", "strip")
    prev = lax.ppermute(x, axes, [(at(t, s), at(t + 1, s)) for t in range(nt - 1) for s in range(ns)])
    both = jnp.concatenate([prev, x], axis=0)
    odd = lax.axis_index("strip") % 2 == 1
    top, bottom = both[:, :2], both[:, 10:]
    outer = lax.ppermute(jnp.where(odd, bottom, top), axes,
                         [(at(t, s), at(t, s + 1 if s % 2 else s - 1)) for t in range(nt) for s in range(1, ns - 1)])
    inner = lax.ppermute(jnp.where(odd, top, bottom), axes,
                         [(at(t, s), at(t, s ^ 1)) for t in range(nt) for s in range(ns - ns % 2)])
    vm = pl.BlockSpec(memory_space=pltpu.VMEM)
    two = lambda v: v.reshape(1, -1)
    w4, wv, part = pl.pallas_call(
        own,
        out_shape=(jax.ShapeDtypeStruct((4 * c0, 4 * c1), BF), jax.ShapeDtypeStruct(wc.shape, BF),
                   jax.ShapeDtypeStruct((256, c0), F32)),
        in_specs=[vm, vm, pl.BlockSpec(memory_space=pltpu.HBM), vm],
        out_specs=(vm, vm, vm),
        scratch_shapes=[
            pltpu.VMEM((4 * c1, 4 * c0), BF),
            pltpu.VMEM((3, 272, 128), F32),
            pltpu.VMEM((3, 256, c0), BF),
            pltpu.SemaphoreType.DMA((3,)),
        ],
        compiler_params=pltpu.CompilerParams(vmem_limit_bytes=26 << 20),
    )(x, two(gain0), pltpu.with_memory_space_constraint(wc, pltpu.HBM), jnp.swapaxes(wu, 2, 3))
    return pl.pallas_call(
        functools.partial(kernel, ns - 1),
        out_shape=jax.ShapeDtypeStruct((4, 24, 8, c1), BF),
        in_specs=[vm] * 12,
        out_specs=vm,
        scratch_shapes=[
            pltpu.VMEM((3, 336, 128), F32),
            pltpu.VMEM((3, 384, c0), BF),
            pltpu.VMEM((3, 3, 64, c0), BF),
            pltpu.VMEM((3, 64, 128), F32),
            pltpu.VMEM((400, c0), F32),
            pltpu.VMEM((2, 5, 112, 2 * c1), F32),
            pltpu.VMEM((2, 2, 5, 96, 2 * c1), BF),
            pltpu.VMEM((2, 32, 2 * c1), F32),
            pltpu.VMEM((2, 768, 128), F32),
        ],
        compiler_params=pltpu.CompilerParams(vmem_limit_bytes=14 << 20),
    )(part, prev, outer, inner, two(gain0), wv, two(bias0), w4, two(bias1), two(gain1), wf, two(bias2))


def solution(mesh):
    nt, ns = mesh.shape["tm"], mesh.shape["strip"]
    part = P("tm", "strip", None, None)
    return jax.shard_map(
        functools.partial(block, nt=nt, ns=ns), mesh=mesh,
        in_specs=(part,) + (P(),) * 8, out_specs=part, check_vma=False)
```

```python
import functools

import jax
import jax.numpy as jnp
from jax import lax
from jax.experimental import pallas as pl
from jax.experimental.pallas import tpu as pltpu
from jax.sharding import PartitionSpec as P


EPS = 1e-6
BF = jnp.bfloat16
F32 = jnp.float32


def silu(v):
    half = 0.5 * v
    return half + half * jnp.tanh(half)


def dot(a, b):
    return jnp.dot(a, b, preferred_element_type=F32)


def phases(wu, w4, turned):
    c1, c0 = wu.shape[2:]
    for r in range(0, c1, 16):
        f = [[wu[kh, kw, r:r + 16, :].astype(F32) for kw in range(3)] for kh in range(3)]
        cols = [[(k[0], k[1] + k[2]), (k[0] + k[1], k[2])] for k in f]
        for wcol in range(2):
            tap = [[cols[kh][b][wcol] for b in range(2)] for kh in range(3)]
            first = tap[0] + [tap[0][b] + tap[1][b] for b in range(2)]
            second = [tap[1][b] + tap[2][b] for b in range(2)] + tap[2]
            for hrow, parts in enumerate((first, second)):
                at = (2 * wcol + hrow) * c0
                for i, v in enumerate(parts):
                    turned[c1 * i + r:c1 * i + r + 16, at:at + c0] = v.astype(BF)
    for k in range(0, 4 * c0, 128):
        w4[k:k + 128, :] = turned[:, k:k + 128].T


def put(raw, row, v):
    for c in range(3):
        raw[c, row:row + v.shape[0], :] = v[:, 128 * c:128 * c + 128]


def normed(raw, row, g0):
    v = jnp.concatenate([raw[c, row:row + 64, :] for c in range(3)], axis=1)
    r = lax.rsqrt(jnp.mean(v * v, axis=-1, keepdims=True) + EPS)
    return silu(v * r * g0)


def spread(raw, left, t):
    for kh in range(3):
        for w in range(4):
            for c in range(3):
                v = raw[c, pl.ds(64 * t + 4 * kh + w, 16, stride=4), :]
                left[kh, 64 * t + 16 * w:64 * t + 16 * w + 16, 128 * c:128 * c + 128] = v.astype(BF)


SPAN = ((0, 3), (0, 4), (1, 3))


def blank(raw, n):
    zero = jnp.zeros((8, 3 * raw.shape[-1]), F32)
    for t in range(n):
        put(raw, 64 * t, zero)
        put(raw, 64 * t + 56, zero)
    put(raw, 64 * n, zero)


def gather(left, lo, m, first, n):
    return jnp.concatenate(
        [jnp.concatenate([left[kh, 64 * t + 16 * lo:64 * t + 16 * (lo + m), :] for t in range(first, first + n)], axis=0)
         for kh in range(3)], axis=1)


def stack(wc, kt, kw):
    return jnp.concatenate([wc[kt, kh, kw] for kh in range(3)], axis=0)


def own(x_hbm, gain0, wc, wu_hbm, w4, wv, part, x, wu, turned, raw, left, sems):
    c0 = x.shape[-1]
    get_x = pltpu.make_async_copy(x_hbm, x, sems.at[3])
    get_x.start()
    get_u = pltpu.make_async_copy(wu_hbm, wu, sems.at[4])
    get_u.start()
    copies = {}
    for kt in (2, 1, 0):
        copies[kt] = pltpu.make_async_copy(wc.at[kt], wv.at[kt], sems.at[kt])
        copies[kt].start()
    g0 = gain0[...].reshape(1, c0)
    blank(raw, 4)
    get_x.wait()
    for t in range(4):
        for h in range(12):
            put(raw, 64 * t + 8 + 4 * h, x[t, h].astype(F32))
        put(raw, 64 * t, normed(raw, 64 * t, g0))
    for t in range(4):
        spread(raw, left, t)
    get_u.wait()
    phases(wu, w4, turned)
    for kt in (2, 1, 0):
        copies[kt].wait()
        n = kt + 2
        for kw in (1, 0, 2):
            lo, m = SPAN[kw]
            d = dot(gather(left, lo, m, 0, n), stack(wv, kt, kw))
            for t in range(n):
                at = 64 * (t + 2 - kt) + 16 * (lo + 1 - kw)
                v = d[16 * m * t:16 * m * (t + 1)]
                if kt == 2 and kw == 1:
                    part[at:at + 16 * m, :] = v
                else:
                    part[at:at + 16 * m, :] += v


def old(part, prev, gain0, wc, bias0, mid, raw, left):
    c0 = prev.shape[-1]
    g0 = gain0[...].reshape(1, c0)
    b0 = bias0[...].reshape(1, c0)
    blank(raw, 4)
    for t in range(4):
        for h in range(12):
            put(raw, 64 * t + 8 + 4 * h, prev[t, h].astype(F32))
        put(raw, 64 * t, normed(raw, 64 * t, g0))
    for t in range(4):
        spread(raw, left, t)
    mid[0:128, :] = jnp.broadcast_to(b0, (128, c0))
    mid[128:384, :] = part[...] + b0
    for kt in range(3):
        n = 4 - kt
        for kw in range(3):
            lo, m = SPAN[kw]
            d = dot(gather(left, lo, m, kt, n), stack(wc, kt, kw))
            for u in range(n):
                at = 64 * u + 16 * (lo + 1 - kw)
                mid[at:at + 16 * m, :] += d[16 * m * u:16 * m * (u + 1)]


def kernel(last, sums, inner, outer, gain0, wc, w4, bias1, gain1, wf, bias2, out,
           raw, left, ends, tail, mid, lift, planes, nat, back):
    group = lax.axis_index("tm")
    strip = lax.axis_index("strip")
    c0 = wc.shape[-1]
    c1 = wf.shape[-1]
    odd = strip % 2 == 1

    for t in range(8):
        for i in range(2):
            a, b = inner[t, i].astype(F32), outer[t, i].astype(F32)
            put(raw, 16 * t + 4 * i, jnp.where(odd, a, b))
            put(raw, 16 * t + 8 + 4 * i, jnp.where(odd, b, a))
    g0 = gain0[...].reshape(1, c0)
    row = lax.broadcasted_iota(jnp.int32, (8, c0), 0)
    none = jnp.zeros((8, c0), F32)
    for half in range(2):
        v = normed(raw, 64 * half, g0)
        for i in range(4):
            t = 4 * half + i
            up, down = v[16 * i:16 * i + 8], v[16 * i + 8:16 * i + 16]
            for kh in range(3):
                a = (up, jnp.where(row < 4, pltpu.roll(up, 4, 0), 0.0), none)[kh]
                b = (none, jnp.where(row < 4, 0.0, pltpu.roll(down, 4, 0)), down)[kh]
                for kw in range(3):
                    if kw == 0:
                        e = [jnp.where(row % 4 == 0, 0.0, pltpu.roll(z, 1, 0)) for z in (a, b)]
                    elif kw == 2:
                        e = [jnp.where(row % 4 == 3, 0.0, pltpu.roll(z, 7, 0)) for z in (a, b)]
                    else:
                        e = [a, b]
                    ends[kw, kh, 16 * t:16 * t + 16, :] = jnp.concatenate(e, axis=0).astype(BF)
    every = [(kt, kw, kh) for kt in range(3) for kw in range(3) for kh in range(3)]
    d = dot(jnp.concatenate([ends[kw, kh, 16 * kt:16 * kt + 96, :] for kt, kw, kh in every], axis=1),
            jnp.concatenate([wc[kt, kh, kw] for kt, kw, kh in every], axis=0))
    for c in range(3):
        tail[c] = d[:, 128 * c:128 * c + 128]
    mid[0:384, :] = sums[...]
    for t in range(6):
        for w in range(4):
            for c in range(3):
                for i, r in enumerate((0, 12)):
                    at = 64 * t + 16 * w + r
                    mid[at:at + 2, 128 * c:128 * c + 128] += tail[c, pl.ds(16 * t + 8 * i + w, 2, stride=4), :]
    row = lax.broadcasted_iota(jnp.int32, (16, c0), 0)
    keep = jnp.logical_and(jnp.logical_or(strip > 0, row != 0), jnp.logical_or(strip < last, row != 13))
    for t in range(6):
        for w in range(4):
            at = 64 * t + 16 * w
            v = jnp.where(keep, mid[at:at + 16, :], 0.0)
            mid[at:at + 16, :] = v
    for t in range(6):
        for w in range(4):
            at = 64 * t + 16 * w
            left[0, at:at + 16, :] = mid[at:at + 16, :].astype(BF)
            left[1, at:at + 16, :] = mid[at + 1:at + 17, :].astype(BF)

    def ups(lo, n):
        a = jnp.concatenate([left[0, 64 * t + 16 * lo:64 * t + 16 * (lo + n), :] for t in range(6)], axis=0)
        b = jnp.concatenate([left[1, 64 * t + 16 * lo:64 * t + 16 * (lo + n), :] for t in range(6)], axis=0)
        return jnp.concatenate([a, b], axis=1)

    b1 = bias1[...]
    b1 = jnp.concatenate([b1, b1], axis=1)
    g1 = gain1[...]
    g1 = jnp.concatenate([g1, g1], axis=1)
    lane = lax.broadcasted_iota(jnp.int32, (16, 2 * c1), 1)
    even = lane < c1
    row = lax.broadcasted_iota(jnp.int32, (16, 2 * c1), 0)

    def finish(u, p, t, a):
        l = (u + b1).astype(BF).astype(F32)
        lift[a, p, 16 * t:16 * t + 16, :] = l
        sq = l * l
        me = jnp.sum(jnp.where(even, sq, 0.0), axis=-1, keepdims=True) * (1.0 / c1)
        mo = jnp.sum(jnp.where(even, 0.0, sq), axis=-1, keepdims=True) * (1.0 / c1)
        r = jnp.where(even, lax.rsqrt(me + EPS), lax.rsqrt(mo + EPS))
        v = silu(l * r * g1)
        if p == 0:
            v = jnp.where(even, v, 0.0)
        if p == 4:
            v = jnp.where(even, 0.0, v)
        if a == 0:
            ok = jnp.logical_or(strip < last, row != 12)
        else:
            ok = jnp.logical_or(strip > 0, row != 0)
        if t < 2:
            ok = jnp.logical_and(ok, group > 0)
        nat[a, 0:16, 0:2 * c1] = jnp.where(ok, v, 0.0)
        planes[a, 0, p, 16 * t:16 * t + 16, :] = nat[a, 0:16, 0:2 * c1].astype(BF)
        planes[a, 1, p, 16 * t:16 * t + 16, :] = nat[a, 1:17, 0:2 * c1].astype(BF)

    u = dot(jnp.concatenate([ups(0, 3), ups(1, 3)], axis=1), w4[...])
    for t in range(6):
        for p in range(1, 4):
            for a in range(2):
                finish(u[48 * t + 16 * p - 16:48 * t + 16 * p, 2 * c1 * a:2 * c1 * (a + 1)], p, t, a)
    u = dot(ups(0, 1), w4[2 * c0:, :])
    for t in range(6):
        for a in range(2):
            finish(u[16 * t:16 * t + 16, 2 * c1 * a:2 * c1 * (a + 1)], 0, t, a)
    u = dot(ups(3, 1), w4[:2 * c0, :])
    for t in range(6):
        for a in range(2):
            finish(u[16 * t:16 * t + 16, 2 * c1 * a:2 * c1 * (a + 1)], 4, t, a)

    b2 = bias2[...]
    zero = jnp.zeros((64, c1), BF)
    for a in range(2):
        reads = ((1, 0), (0, 0), (1, 1)) if a == 0 else ((0, 0), (1, 1), (0, 1))
        for b in range(2):
            cols, rhs = [], []
            for kt in range(3):
                for kh in range(3):
                    ph, sh = reads[kh]
                    first = jnp.concatenate([planes[ph, sh, q, 16 * kt:16 * kt + 64, :] for q in range(4)], axis=0)
                    second = jnp.concatenate([planes[ph, sh, q + 1, 16 * kt:16 * kt + 64, :] for q in range(4)], axis=0)
                    k0, k1, k2 = (wf[kt, kh, kw] for kw in range(3))
                    if b == 0:
                        cols += [first, second[:, 128:]]
                        rhs += [k1, k0, zero, k2]
                    else:
                        cols += [first[:, :256], second]
                        rhs += [k0, zero, k2, k1]
            d = dot(jnp.concatenate(cols, axis=1), jnp.concatenate(rhs, axis=0)) + b2
            for q in range(4):
                for t in range(4):
                    p = q if b == 0 else q + 1
                    at = 16 * (t + 2) + a
                    l = lift[a, p, at:at + 12, :]
                    l = l[:, :c1] if b == 0 else l[:, c1:]
                    v = d[64 * q + 16 * t:64 * q + 16 * t + 12, :] + l
                    nat_rows = pl.ds((24 * t + a) * 8 + 2 * q + b, 12, stride=16)
                    back[0, nat_rows, :] = v[:, :128]
                    back[1, nat_rows, 0:64] = v[:, 128:]
    for t in range(4):
        v = jnp.concatenate([back[0, 192 * t:192 * t + 192, :], back[1, 192 * t:192 * t + 192, 0:64]], axis=1)
        out[t] = v.reshape(24, 8, c1).astype(BF)


def block(x, gain0, wc, bias0, wu, bias1, gain1, wf, bias2, *, nt, ns):
    c0, c1 = wc.shape[-1], wf.shape[-1]
    at = lambda t, s: t * ns + s
    vm = pl.BlockSpec(memory_space=pltpu.VMEM)
    hbm = pl.BlockSpec(memory_space=pltpu.HBM)
    far = lambda v: pltpu.with_memory_space_constraint(v, pltpu.HBM)
    two = lambda v: v.reshape(1, -1)
    axes = ("tm", "strip")
    prev = lax.ppermute(x, axes, [(at(t, s), at(t + 1, s)) for t in range(nt - 1) for s in range(ns)])
    w4, wv, part = pl.pallas_call(
        own,
        out_shape=(jax.ShapeDtypeStruct((4 * c0, 4 * c1), BF), jax.ShapeDtypeStruct(wc.shape, BF),
                   jax.ShapeDtypeStruct((256, c0), F32)),
        in_specs=[hbm, vm, hbm, hbm],
        out_specs=(vm, vm, vm),
        scratch_shapes=[
            pltpu.VMEM(x.shape, BF),
            pltpu.VMEM((3, 3, c1, c0), BF),
            pltpu.VMEM((4 * c1, 4 * c0), BF),
            pltpu.VMEM((3, 272, 128), F32),
            pltpu.VMEM((3, 256, c0), BF),
            pltpu.SemaphoreType.DMA((5,)),
        ],
        compiler_params=pltpu.CompilerParams(vmem_limit_bytes=26 << 20),
    )(far(x), gain0, far(wc), far(jnp.swapaxes(wu, 2, 3)))
    both = jnp.concatenate([prev, x], axis=0)
    odd = lax.axis_index("strip") % 2 == 1
    top, bottom = both[:, :2], both[:, 10:]
    inner = lax.ppermute(jnp.where(odd, top, bottom), axes,
                         [(at(t, s), at(t, s ^ 1)) for t in range(nt) for s in range(ns)])
    outer = lax.ppermute(jnp.where(odd, bottom, top), axes,
                         [(at(t, s), at(t, s + 1 if s % 2 else s - 1)) for t in range(nt) for s in range(1, ns - 1)])
    sums = pl.pallas_call(
        old,
        out_shape=jax.ShapeDtypeStruct((384, c0), F32),
        in_specs=[vm] * 5,
        out_specs=vm,
        scratch_shapes=[pltpu.VMEM((3, 272, 128), F32), pltpu.VMEM((3, 256, c0), BF)],
        compiler_params=pltpu.CompilerParams(vmem_limit_bytes=14 << 20),
    )(part, prev, gain0, wv, bias0)
    return pl.pallas_call(
        functools.partial(kernel, ns - 1),
        out_shape=jax.ShapeDtypeStruct((4, 24, 8, c1), BF),
        in_specs=[vm] * 10,
        out_specs=vm,
        scratch_shapes=[
            pltpu.VMEM((3, 128, 128), F32),
            pltpu.VMEM((2, 384, c0), BF),
            pltpu.VMEM((3, 3, 128, c0), BF),
            pltpu.VMEM((3, 96, 128), F32),
            pltpu.VMEM((400, c0), F32),
            pltpu.VMEM((2, 5, 112, 2 * c1), F32),
            pltpu.VMEM((2, 2, 5, 96, 2 * c1), BF),
            pltpu.VMEM((2, 32, 2 * c1), F32),
            pltpu.VMEM((2, 768, 128), F32),
        ],
        compiler_params=pltpu.CompilerParams(vmem_limit_bytes=14 << 20),
    )(sums, inner, outer, gain0, wv, w4, two(bias1), two(gain1), wf, two(bias2))


def solution(mesh):
    nt, ns = mesh.shape["tm"], mesh.shape["strip"]
    part = P("tm", "strip", None, None)
    return jax.shard_map(
        functools.partial(block, nt=nt, ns=ns), mesh=mesh,
        in_specs=(part,) + (P(),) * 8, out_specs=part, check_vma=False)
```

```python
import functools

import jax
import jax.numpy as jnp
from jax import lax
from jax.experimental import pallas as pl
from jax.experimental.pallas import tpu as pltpu
from jax.sharding import PartitionSpec as P


EPS = 1e-6
BF = jnp.bfloat16
F32 = jnp.float32


def silu(v):
    half = 0.5 * v
    return half + half * jnp.tanh(half)


def dot(a, b):
    return jnp.dot(a, b, preferred_element_type=F32)


def phases(wu, w4, turned):
    c1, c0 = wu.shape[2:]
    for r in range(0, c1, 16):
        f = [[wu[kh, kw, r:r + 16, :].astype(F32) for kw in range(3)] for kh in range(3)]
        cols = [[(k[0], k[1] + k[2]), (k[0] + k[1], k[2])] for k in f]
        for wcol in range(2):
            tap = [[cols[kh][b][wcol] for b in range(2)] for kh in range(3)]
            first = tap[0] + [tap[0][b] + tap[1][b] for b in range(2)]
            second = [tap[1][b] + tap[2][b] for b in range(2)] + tap[2]
            for hrow, parts in enumerate((first, second)):
                at = (2 * wcol + hrow) * c0
                for i, v in enumerate(parts):
                    turned[c1 * i + r:c1 * i + r + 16, at:at + c0] = v.astype(BF)
    for k in range(0, 4 * c0, 128):
        w4[k:k + 128, :] = turned[:, k:k + 128].T


def put(raw, row, v):
    for c in range(3):
        raw[c, row:row + v.shape[0], :] = v[:, 128 * c:128 * c + 128]


def normed(raw, row, g0):
    v = jnp.concatenate([raw[c, row:row + 64, :] for c in range(3)], axis=1)
    r = lax.rsqrt(jnp.mean(v * v, axis=-1, keepdims=True) + EPS)
    return silu(v * r * g0)


def spread(raw, left, t):
    for kh in range(3):
        for w in range(4):
            for c in range(3):
                v = raw[c, pl.ds(64 * t + 4 * kh + w, 16, stride=4), :]
                left[kh, 64 * t + 16 * w:64 * t + 16 * w + 16, 128 * c:128 * c + 128] = v.astype(BF)


SPAN = ((0, 3), (0, 4), (1, 3))


def blank(raw, n):
    zero = jnp.zeros((8, 3 * raw.shape[-1]), F32)
    for t in range(n):
        put(raw, 64 * t, zero)
        put(raw, 64 * t + 56, zero)
    put(raw, 64 * n, zero)


def gather(left, lo, m, first, n):
    return jnp.concatenate(
        [jnp.concatenate([left[kh, 64 * t + 16 * lo:64 * t + 16 * (lo + m), :] for t in range(first, first + n)], axis=0)
         for kh in range(3)], axis=1)


def stack(wc, kt, kw):
    return jnp.concatenate([wc[kt, kh, kw] for kh in range(3)], axis=0)


def own(x_hbm, gain0, wc, wu_hbm, w4, wv, part, x, wu, turned, raw, left, sems):
    c0 = x.shape[-1]
    get_x = pltpu.make_async_copy(x_hbm, x, sems.at[3])
    get_x.start()
    get_u = pltpu.make_async_copy(wu_hbm, wu, sems.at[4])
    get_u.start()
    copies = {}
    for kt in (2, 1, 0):
        copies[kt] = pltpu.make_async_copy(wc.at[kt], wv.at[kt], sems.at[kt])
        copies[kt].start()
    g0 = gain0[...].reshape(1, c0)
    blank(raw, 4)
    get_x.wait()
    for t in range(4):
        for h in range(12):
            put(raw, 64 * t + 8 + 4 * h, x[t, h].astype(F32))
        put(raw, 64 * t, normed(raw, 64 * t, g0))
    for t in range(4):
        spread(raw, left, t)
    get_u.wait()
    phases(wu, w4, turned)
    for kt in (2, 1, 0):
        copies[kt].wait()
        n = kt + 2
        for kw in (1, 0, 2):
            lo, m = SPAN[kw]
            d = dot(gather(left, lo, m, 0, n), stack(wv, kt, kw))
            for t in range(n):
                at = 64 * (t + 2 - kt) + 16 * (lo + 1 - kw)
                v = d[16 * m * t:16 * m * (t + 1)]
                if kt == 2 and kw == 1:
                    part[at:at + 16 * m, :] = v
                else:
                    part[at:at + 16 * m, :] += v


def old(part, prev, gain0, wc, bias0, mid, raw, left):
    c0 = prev.shape[-1]
    g0 = gain0[...].reshape(1, c0)
    b0 = bias0[...].reshape(1, c0)
    blank(raw, 4)
    for t in range(4):
        for h in range(12):
            put(raw, 64 * t + 8 + 4 * h, prev[t, h].astype(F32))
        put(raw, 64 * t, normed(raw, 64 * t, g0))
    for t in range(4):
        spread(raw, left, t)
    mid[0:128, :] = jnp.broadcast_to(b0, (128, c0))
    mid[128:384, :] = part[...] + b0
    for kt in range(3):
        n = 4 - kt
        for kw in range(3):
            lo, m = SPAN[kw]
            d = dot(gather(left, lo, m, kt, n), stack(wc, kt, kw))
            for u in range(n):
                at = 64 * u + 16 * (lo + 1 - kw)
                mid[at:at + 16 * m, :] += d[16 * m * u:16 * m * (u + 1)]


def kernel(last, sums, inner, outer, gain0, wc, w4, bias1, gain1, wf, bias2, out,
           raw, left, ends, tail, mid, lift, lines, planes, back):
    group = lax.axis_index("tm")
    strip = lax.axis_index("strip")
    c0 = wc.shape[-1]
    c1 = wf.shape[-1]
    odd = strip % 2 == 1

    for t in range(8):
        for i in range(2):
            a, b = inner[t, i].astype(F32), outer[t, i].astype(F32)
            put(raw, 16 * t + 4 * i, jnp.where(odd, a, b))
            put(raw, 16 * t + 8 + 4 * i, jnp.where(odd, b, a))
    g0 = gain0[...].reshape(1, c0)
    row = lax.broadcasted_iota(jnp.int32, (8, c0), 0)
    none = jnp.zeros((8, c0), F32)
    for half in range(2):
        v = normed(raw, 64 * half, g0)
        for i in range(4):
            t = 4 * half + i
            up, down = v[16 * i:16 * i + 8], v[16 * i + 8:16 * i + 16]
            for kh in range(3):
                a = (up, jnp.where(row < 4, pltpu.roll(up, 4, 0), 0.0), none)[kh]
                b = (none, jnp.where(row < 4, 0.0, pltpu.roll(down, 4, 0)), down)[kh]
                for kw in range(3):
                    if kw == 0:
                        e = [jnp.where(row % 4 == 0, 0.0, pltpu.roll(z, 1, 0)) for z in (a, b)]
                    elif kw == 2:
                        e = [jnp.where(row % 4 == 3, 0.0, pltpu.roll(z, 7, 0)) for z in (a, b)]
                    else:
                        e = [a, b]
                    ends[kw, kh, 16 * t:16 * t + 16, :] = jnp.concatenate(e, axis=0).astype(BF)
    every = [(kt, kw, kh) for kt in range(3) for kw in range(3) for kh in range(3)]
    d = dot(jnp.concatenate([ends[kw, kh, 16 * kt:16 * kt + 96, :] for kt, kw, kh in every], axis=1),
            jnp.concatenate([wc[kt, kh, kw] for kt, kw, kh in every], axis=0))
    for c in range(3):
        tail[c, 8:104, :] = d[:, 128 * c:128 * c + 128]
    sub = lax.broadcasted_iota(jnp.int32, (8, 128), 0)
    keep_top = jnp.logical_or(strip > 0, sub != 0)
    keep_end = jnp.logical_or(strip < last, sub != 5)
    for t in range(6):
        for w in range(4):
            at = 64 * t + 16 * w
            for c in range(3):
                lanes = slice(128 * c, 128 * c + 128)
                top = sums[at:at + 8, lanes] + jnp.where(sub < 2, tail[c, pl.ds(16 * t + w + 8, 8, stride=4), :], 0.0)
                add = jnp.where(sub // 2 == 2, tail[c, pl.ds(16 * t + w, 8, stride=4), :], 0.0)
                end = sums[at + 8:at + 16, lanes] + add
                v = jnp.concatenate([jnp.where(keep_top, top, 0.0), jnp.where(keep_end, end, 0.0)], axis=0)
                mid[c, at:at + 16, :] = v
                left[0, at:at + 16, lanes] = v.astype(BF)
    for at in range(0, 384, 16):
        for c in range(3):
            left[1, at:at + 16, 128 * c:128 * c + 128] = mid[c, at + 1:at + 17, :].astype(BF)

    def ups(lo, n, first, count):
        both = [jnp.concatenate([left[i, 64 * t + 16 * lo:64 * t + 16 * (lo + n), :] for t in range(first, first + count)],
                                axis=0) for i in range(2)]
        return jnp.concatenate(both, axis=1)

    def thirds(v):
        v = jnp.concatenate([v, v], axis=1)
        return [v[:, 128 * c:128 * c + 128] for c in range(3)]

    b1 = thirds(bias1[...])
    g1 = thirds(0.5 * gain1[...])
    low = lax.broadcasted_iota(jnp.int32, (16, 128), 1) < 64
    row = lax.broadcasted_iota(jnp.int32, (16, 1), 0)
    ok_end = jnp.logical_or(strip < last, row != 12)
    ok_top = jnp.logical_or(strip > 0, row != 0)
    early = [jnp.logical_and(ok, group > 0) for ok in (ok_end, ok_top)]

    def finish(u, p, t, a):
        l = [(u[:, 128 * c:128 * c + 128] + b1[c]).astype(BF).astype(F32) for c in range(3)]
        at = 16 * t
        for c in range(3):
            lift[a, p, c, at:at + 16, :] = l[c]
        ok = early[a] if t < 2 else (ok_end, ok_top)[a]
        mids = l[1] * l[1]
        part = jnp.where(low, mids, 0.0)
        none = jnp.zeros((16, 1), F32)
        re = ro = none
        if p < 4:
            re = jnp.sum(l[0] * l[0] + part, axis=-1, keepdims=True) * (1.0 / c1)
            re = jnp.where(ok, lax.rsqrt(re + EPS), 0.0)
        if p > 0:
            ro = jnp.sum(l[2] * l[2] + (mids - part), axis=-1, keepdims=True) * (1.0 / c1)
            ro = jnp.where(ok, lax.rsqrt(ro + EPS), 0.0)
        for c, r in enumerate((re, jnp.where(low, re, ro), ro)):
            if r is none:
                lines[a, p, c, at:at + 16, :] = jnp.zeros((16, 128), F32)
            else:
                h = l[c] * (r * g1[c])
                lines[a, p, c, at:at + 16, :] = h + h * jnp.tanh(h)

    def dense(ref, s, kt):
        rows = lambda t, k: ref[16 * t + s + k:16 * t + s + k + 8, :]
        seam = lambda t: jnp.where(sub < 4, rows(t, 8), rows(t + 1, -4))
        return jnp.concatenate(
            [rows(kt, 0), seam(kt), rows(kt + 1, 4), rows(kt + 2, 0), seam(kt + 2), rows(kt + 3, 4)], axis=0)

    def pack(p):
        for a in range(2):
            for s in range(2):
                for kt in range(3):
                    for c in range(3):
                        planes[a, s, p, kt, :, 128 * c:128 * c + 128] = dense(lines.at[a, p, c], s, kt).astype(BF)

    u0 = dot(ups(0, 1, 0, 6), w4[2 * c0:, :])
    u4 = dot(ups(3, 1, 0, 6), w4[:2 * c0, :])
    chunks = [dot(jnp.concatenate([ups(0, 3, 0, 3), ups(1, 3, 0, 3)], axis=1), w4[...])]
    for p, u in ((0, u0), (4, u4)):
        for t in range(6):
            for a in range(2):
                finish(u[16 * t:16 * t + 16, 2 * c1 * a:2 * c1 * (a + 1)], p, t, a)
        pack(p)
    chunks.append(dot(jnp.concatenate([ups(0, 3, 3, 3), ups(1, 3, 3, 3)], axis=1), w4[...]))
    for i in range(2):
        for t in range(3):
            for p in range(1, 4):
                at = 48 * t + 16 * (p - 1)
                for a in range(2):
                    finish(chunks[i][at:at + 16, 2 * c1 * a:2 * c1 * (a + 1)], p, 3 * i + t, a)
    for p in range(1, 4):
        pack(p)

    b2 = bias2[...]
    zero = jnp.zeros((64, c1), BF)
    for a in range(2):
        reads = ((1, 0), (0, 0), (1, 1)) if a == 0 else ((0, 0), (1, 1), (0, 1))
        for b in (1, 0):
            cols, rhs = [], []
            for kt in range(3):
                for kh in range(3):
                    ph, sh = reads[kh]
                    first = jnp.concatenate([planes[ph, sh, q, kt] for q in range(4)], axis=0)
                    second = jnp.concatenate([planes[ph, sh, q + 1, kt] for q in range(4)], axis=0)
                    k0, k1, k2 = (wf[kt, kh, kw] for kw in range(3))
                    if b == 0:
                        cols += [first, second[:, 128:]]
                        rhs += [k1, k0, zero, k2]
                    else:
                        cols += [first[:, :256], second]
                        rhs += [k0, zero, k2, k1]
            d = dot(jnp.concatenate(cols, axis=1), jnp.concatenate(rhs, axis=0))
            for q in range(4):
                l = jnp.concatenate([dense(lift.at[a, q + b, b + c], a, 2) for c in range(2)], axis=1)
                v = d[48 * q:48 * q + 48] + ((l[:, 64:] if b else l[:, :c1]) + b2)
                back[a, 0, pl.ds(2 * q + b, 48, stride=8), :] = v[:, :128]
                back[a, 1, pl.ds(2 * q + b, 48, stride=8), 0:64] = v[:, 128:]
        for t in range(4):
            for i in range(12):
                at = 96 * t + 8 * i
                out[t, 2 * i + a] = jnp.concatenate([back[a, 0, at:at + 8, :], back[a, 1, at:at + 8, 0:64]], axis=1).astype(BF)


def block(x, gain0, wc, bias0, wu, bias1, gain1, wf, bias2, *, nt, ns):
    c0, c1 = wc.shape[-1], wf.shape[-1]
    at = lambda t, s: t * ns + s
    vm = pl.BlockSpec(memory_space=pltpu.VMEM)
    hbm = pl.BlockSpec(memory_space=pltpu.HBM)
    far = lambda v: pltpu.with_memory_space_constraint(v, pltpu.HBM)
    two = lambda v: v.reshape(1, -1)
    axes = ("tm", "strip")
    prev = lax.ppermute(x, axes, [(at(t, s), at(t + 1, s)) for t in range(nt - 1) for s in range(ns)])
    w4, wv, part = pl.pallas_call(
        own,
        out_shape=(jax.ShapeDtypeStruct((4 * c0, 4 * c1), BF), jax.ShapeDtypeStruct(wc.shape, BF),
                   jax.ShapeDtypeStruct((256, c0), F32)),
        in_specs=[hbm, vm, hbm, hbm],
        out_specs=(vm, vm, vm),
        scratch_shapes=[
            pltpu.VMEM(x.shape, BF),
            pltpu.VMEM((3, 3, c1, c0), BF),
            pltpu.VMEM((4 * c1, 4 * c0), BF),
            pltpu.VMEM((3, 272, 128), F32),
            pltpu.VMEM((3, 256, c0), BF),
            pltpu.SemaphoreType.DMA((5,)),
        ],
        compiler_params=pltpu.CompilerParams(vmem_limit_bytes=26 << 20),
    )(far(x), gain0, far(wc), far(jnp.swapaxes(wu, 2, 3)))
    both = jnp.concatenate([prev, x], axis=0)
    odd = lax.axis_index("strip") % 2 == 1
    top, bottom = both[:, :2], both[:, 10:]
    inner = lax.ppermute(jnp.where(odd, top, bottom), axes,
                         [(at(t, s), at(t, s ^ 1)) for t in range(nt) for s in range(ns)])
    outer = lax.ppermute(jnp.where(odd, bottom, top), axes,
                         [(at(t, s), at(t, s + 1 if s % 2 else s - 1)) for t in range(nt) for s in range(1, ns - 1)])
    sums = pl.pallas_call(
        old,
        out_shape=jax.ShapeDtypeStruct((384, c0), F32),
        in_specs=[vm] * 5,
        out_specs=vm,
        scratch_shapes=[pltpu.VMEM((3, 272, 128), F32), pltpu.VMEM((3, 256, c0), BF)],
        compiler_params=pltpu.CompilerParams(vmem_limit_bytes=14 << 20),
    )(part, prev, gain0, wv, bias0)
    return pl.pallas_call(
        functools.partial(kernel, ns - 1),
        out_shape=jax.ShapeDtypeStruct((4, 24, 8, c1), BF),
        in_specs=[vm] * 10,
        out_specs=vm,
        scratch_shapes=[
            pltpu.VMEM((3, 128, 128), F32),
            pltpu.VMEM((2, 384, c0), BF),
            pltpu.VMEM((3, 3, 128, c0), BF),
            pltpu.VMEM((3, 128, 128), F32),
            pltpu.VMEM((3, 400, 128), F32),
            pltpu.VMEM((2, 5, 3, 112, 128), F32),
            pltpu.VMEM((2, 5, 3, 112, 128), F32),
            pltpu.VMEM((2, 2, 5, 3, 48, 2 * c1), BF),
            pltpu.VMEM((2, 2, 384, 128), F32),
        ],
        compiler_params=pltpu.CompilerParams(vmem_limit_bytes=14 << 20),
    )(sums, inner, outer, gain0, wv, w4, two(bias1), two(gain1), wf, two(bias2))


def solution(mesh):
    nt, ns = mesh.shape["tm"], mesh.shape["strip"]
    part = P("tm", "strip", None, None)
    return jax.shard_map(
        functools.partial(block, nt=nt, ns=ns), mesh=mesh,
        in_specs=(part,) + (P(),) * 8, out_specs=part, check_vma=False)
```

```python
import functools

import jax
import jax.numpy as jnp
from jax import lax
from jax.experimental import pallas as pl
from jax.experimental.pallas import tpu as pltpu
from jax.sharding import PartitionSpec as P


EPS = 1e-6
BF = jnp.bfloat16
F32 = jnp.float32


def silu(v):
    half = 0.5 * v
    return half + half * jnp.tanh(half)


def dot(a, b):
    return jnp.dot(a, b, preferred_element_type=F32)


def phases(wu, w4, turned):
    c1, c0 = wu.shape[2:]
    for r in range(0, c1, 16):
        f = [[wu[kh, kw, r:r + 16, :].astype(F32) for kw in range(3)] for kh in range(3)]
        cols = [[(k[0], k[1] + k[2]), (k[0] + k[1], k[2])] for k in f]
        for wcol in range(2):
            tap = [[cols[kh][b][wcol] for b in range(2)] for kh in range(3)]
            first = tap[0] + [tap[0][b] + tap[1][b] for b in range(2)]
            second = [tap[1][b] + tap[2][b] for b in range(2)] + tap[2]
            for hrow, parts in enumerate((first, second)):
                at = (2 * wcol + hrow) * c0
                for i, v in enumerate(parts):
                    turned[c1 * i + r:c1 * i + r + 16, at:at + c0] = v.astype(BF)
    for k in range(0, 4 * c0, 128):
        w4[k:k + 128, :] = turned[:, k:k + 128].T


def put(raw, row, v):
    for c in range(3):
        raw[c, row:row + v.shape[0], :] = v[:, 128 * c:128 * c + 128]


def normed(raw, row, g0):
    v = jnp.concatenate([raw[c, row:row + 64, :] for c in range(3)], axis=1)
    r = lax.rsqrt(jnp.mean(v * v, axis=-1, keepdims=True) + EPS)
    return silu(v * r * g0)


def spread(raw, left, t):
    for kh in range(3):
        for w in range(4):
            for c in range(3):
                v = raw[c, pl.ds(64 * t + 4 * kh + w, 16, stride=4), :]
                left[kh, 64 * t + 16 * w:64 * t + 16 * w + 16, 128 * c:128 * c + 128] = v.astype(BF)


SPAN = ((0, 3), (0, 4), (1, 3))


def blank(raw, n):
    zero = jnp.zeros((8, 3 * raw.shape[-1]), F32)
    for t in range(n):
        put(raw, 64 * t, zero)
        put(raw, 64 * t + 56, zero)
    put(raw, 64 * n, zero)


def gather(left, lo, m, first, n):
    return jnp.concatenate(
        [jnp.concatenate([left[kh, 64 * t + 16 * lo:64 * t + 16 * (lo + m), :] for t in range(first, first + n)], axis=0)
         for kh in range(3)], axis=1)


def stack(wc, kt, kw):
    return jnp.concatenate([wc[kt, kh, kw] for kh in range(3)], axis=0)


def own(x_hbm, gain0_hbm, wc, wu_hbm, w4, wv, part, x, gain0, wu, turned, raw, left, sems):
    c0 = x.shape[-1]
    get_x = pltpu.make_async_copy(x_hbm, x, sems.at[3])
    get_x.start()
    get_g = pltpu.make_async_copy(gain0_hbm, gain0, sems.at[5])
    get_g.start()
    get_u = pltpu.make_async_copy(wu_hbm, wu, sems.at[4])
    get_u.start()
    copies = {}
    for kt in (2, 1, 0):
        copies[kt] = pltpu.make_async_copy(wc.at[kt], wv.at[kt], sems.at[kt])
        copies[kt].start()
    blank(raw, 4)
    get_x.wait()
    get_g.wait()
    g0 = gain0[...].reshape(1, c0)
    for t in range(4):
        for h in range(12):
            put(raw, 64 * t + 8 + 4 * h, x[t, h].astype(F32))
        put(raw, 64 * t, normed(raw, 64 * t, g0))
    for t in range(4):
        spread(raw, left, t)
    get_u.wait()
    phases(wu, w4, turned)
    for kt in (2, 1, 0):
        copies[kt].wait()
        n = kt + 2
        for kw in (1, 0, 2):
            lo, m = SPAN[kw]
            d = dot(gather(left, lo, m, 0, n), stack(wv, kt, kw))
            for t in range(n):
                at = 64 * (t + 2 - kt) + 16 * (lo + 1 - kw)
                v = d[16 * m * t:16 * m * (t + 1)]
                if kt == 2 and kw == 1:
                    part[at:at + 16 * m, :] = v
                else:
                    part[at:at + 16 * m, :] += v


def old(part, prev, gain0, wc, bias0, mid, raw, left):
    c0 = prev.shape[-1]
    g0 = gain0[...].reshape(1, c0)
    b0 = bias0[...].reshape(1, c0)
    blank(raw, 4)
    for t in range(4):
        for h in range(12):
            put(raw, 64 * t + 8 + 4 * h, prev[t, h].astype(F32))
        put(raw, 64 * t, normed(raw, 64 * t, g0))
    for t in range(4):
        spread(raw, left, t)
    mid[0:128, :] = jnp.broadcast_to(b0, (128, c0))
    mid[128:384, :] = part[...] + b0
    for kt in range(3):
        n = 4 - kt
        for kw in range(3):
            lo, m = SPAN[kw]
            d = dot(gather(left, lo, m, kt, n), stack(wc, kt, kw))
            for u in range(n):
                at = 64 * u + 16 * (lo + 1 - kw)
                mid[at:at + 16 * m, :] += d[16 * m * u:16 * m * (u + 1)]


def kernel(last, sums, inner, outer, gain0, wc, w4, bias1, gain1, wf, bias2, out,
           raw, left, ends, tail, mid, lift, lines, planes, back):
    group = lax.axis_index("tm")
    strip = lax.axis_index("strip")
    c0 = wc.shape[-1]
    c1 = wf.shape[-1]
    odd = strip % 2 == 1

    sub = lax.broadcasted_iota(jnp.int32, (8, 128), 0)

    @pl.when(strip >= 0)
    def _():
        for t in range(8):
            for i in range(2):
                a, b = inner[t, i].astype(F32), outer[t, i].astype(F32)
                put(raw, 16 * t + 4 * i, jnp.where(odd, a, b))
                put(raw, 16 * t + 8 + 4 * i, jnp.where(odd, b, a))
        g0 = gain0[...].reshape(1, c0)
        row = lax.broadcasted_iota(jnp.int32, (8, c0), 0)
        none = jnp.zeros((8, c0), F32)
        for half in range(2):
            v = normed(raw, 64 * half, g0)
            for i in range(4):
                t = 4 * half + i
                up, down = v[16 * i:16 * i + 8], v[16 * i + 8:16 * i + 16]
                for kh in range(3):
                    a = (up, jnp.where(row < 4, pltpu.roll(up, 4, 0), 0.0), none)[kh]
                    b = (none, jnp.where(row < 4, 0.0, pltpu.roll(down, 4, 0)), down)[kh]
                    for kw in range(3):
                        if kw == 0:
                            e = [jnp.where(row % 4 == 0, 0.0, pltpu.roll(z, 1, 0)) for z in (a, b)]
                        elif kw == 2:
                            e = [jnp.where(row % 4 == 3, 0.0, pltpu.roll(z, 7, 0)) for z in (a, b)]
                        else:
                            e = [a, b]
                        ends[kw, kh, 16 * t:16 * t + 16, :] = jnp.concatenate(e, axis=0).astype(BF)
        every = [(kt, kw, kh) for kt in range(3) for kw in range(3) for kh in range(3)]
        d = dot(jnp.concatenate([ends[kw, kh, 16 * kt:16 * kt + 96, :] for kt, kw, kh in every], axis=1),
                jnp.concatenate([wc[kt, kh, kw] for kt, kw, kh in every], axis=0))
        for c in range(3):
            tail[c, 8:104, :] = d[:, 128 * c:128 * c + 128]
        keep_top = jnp.logical_or(strip > 0, sub != 0)
        keep_end = jnp.logical_or(strip < last, sub != 5)
        for t in range(6):
            for w in range(4):
                at = 64 * t + 16 * w
                for c in range(3):
                    lanes = slice(128 * c, 128 * c + 128)
                    top = sums[at:at + 8, lanes] + jnp.where(sub < 2, tail[c, pl.ds(16 * t + w + 8, 8, stride=4), :], 0.0)
                    add = jnp.where(sub // 2 == 2, tail[c, pl.ds(16 * t + w, 8, stride=4), :], 0.0)
                    end = sums[at + 8:at + 16, lanes] + add
                    v = jnp.concatenate([jnp.where(keep_top, top, 0.0), jnp.where(keep_end, end, 0.0)], axis=0)
                    mid[c, at:at + 16, :] = v
                    left[0, at:at + 16, lanes] = v.astype(BF)
        for at in range(0, 384, 16):
            for c in range(3):
                left[1, at:at + 16, 128 * c:128 * c + 128] = mid[c, at + 1:at + 17, :].astype(BF)

    def ups(lo, n, first, count):
        both = [jnp.concatenate([left[i, 64 * t + 16 * lo:64 * t + 16 * (lo + n), :] for t in range(first, first + count)],
                                axis=0) for i in range(2)]
        return jnp.concatenate(both, axis=1)

    def thirds(v):
        v = jnp.concatenate([v, v], axis=1)
        return [v[:, 128 * c:128 * c + 128] for c in range(3)]

    b1 = thirds(bias1[...])
    g1 = thirds(0.5 * gain1[...])
    low = lax.broadcasted_iota(jnp.int32, (16, 128), 1) < 64
    row = lax.broadcasted_iota(jnp.int32, (16, 1), 0)
    ok_end = jnp.logical_or(strip < last, row != 12)
    ok_top = jnp.logical_or(strip > 0, row != 0)
    early = [jnp.logical_and(ok, group > 0) for ok in (ok_end, ok_top)]

    def finish(u, p, t, a):
        l = [None if u[c] is None else (u[c] + b1[c]).astype(BF).astype(F32) for c in range(3)]
        at = 16 * t
        for c in range(3):
            if l[c] is not None:
                lift[a, p, c, at:at + 16, :] = l[c]
        ok = early[a] if t < 2 else (ok_end, ok_top)[a]
        mids = l[1] * l[1]
        part = jnp.where(low, mids, 0.0)
        re = ro = jnp.zeros((16, 1), F32)
        if p < 4:
            re = jnp.sum(l[0] * l[0] + part, axis=-1, keepdims=True) * (1.0 / c1)
            re = jnp.where(ok, lax.rsqrt(re + EPS), 0.0)
        if p > 0:
            ro = jnp.sum(l[2] * l[2] + (mids - part), axis=-1, keepdims=True) * (1.0 / c1)
            ro = jnp.where(ok, lax.rsqrt(ro + EPS), 0.0)
        for c, r in enumerate((re, jnp.where(low, re, ro), ro)):
            if l[c] is not None:
                h = l[c] * (r * g1[c])
                lines[a, p, c, at:at + 16, :] = h + h * jnp.tanh(h)

    def dense(ref, s, kt):
        rows = lambda t, k: ref[16 * t + s + k:16 * t + s + k + 8, :]
        seam = lambda t: jnp.where(sub < 4, rows(t, 8), rows(t + 1, -4))
        return jnp.concatenate(
            [rows(kt, 0), seam(kt), rows(kt + 1, 4), rows(kt + 2, 0), seam(kt + 2), rows(kt + 3, 4)], axis=0)

    def pack(p, kts=range(3)):
        for kt in kts:
            for a in range(2):
                for s in range(2):
                    for c in range(3):
                        none = p == 0 and c == 2 or p == 4 and c == 0
                        v = jnp.zeros((48, 128), BF) if none else dense(lines.at[a, p, c], s, kt).astype(BF)
                        planes[a, s, p, kt, :, 128 * c:128 * c + 128] = v

    def edge(p):
        lhs, rhs = (ups(0, 1, 0, 6), slice(2 * c0, 4 * c0)) if p == 0 else (ups(3, 1, 0, 6), slice(0, 2 * c0))
        u = []
        for a in range(2):
            n = 2 * c1 * a + (0 if p == 0 else 128)
            d = dot(lhs, w4[rhs, n:n + 256])
            u.append([d[:, :128], d[:, 128:], None] if p == 0 else [None, d[:, :128], d[:, 128:]])
        return u

    def chunk(first, count):
        return dot(jnp.concatenate([ups(0, 3, first, count), ups(1, 3, first, count)], axis=1), w4[...])

    def finish_edge(u, p):
        for t in range(6):
            for a in range(2):
                finish([v if v is None else v[16 * t:16 * t + 16] for v in u[a]], p, t, a)
        pack(p)

    def finish_chunk(u, first, count):
        for t in range(count):
            for p in range(1, 4):
                at = 48 * t + 16 * (p - 1)
                for a in range(2):
                    n = 2 * c1 * a
                    finish([u[at:at + 16, n + 128 * c:n + 128 * c + 128] for c in range(3)], p, first + t, a)

    ua = chunk(0, 4)
    u0, u4 = edge(0), edge(4)
    finish_chunk(ua, 0, 4)
    ub = chunk(4, 2)
    for p in range(1, 4):
        pack(p, (0,))
    finish_edge(u0, 0)
    finish_edge(u4, 4)
    finish_chunk(ub, 4, 2)
    for p in range(1, 4):
        pack(p, (1, 2))
    b2 = bias2[...]
    zero = jnp.zeros((64, c1), BF)
    for a in range(2):
        reads = ((1, 0), (0, 0), (1, 1)) if a == 0 else ((0, 0), (1, 1), (0, 1))
        for b in (1, 0):
            cols, rhs = [], []
            for kt in range(3):
                for kh in range(3):
                    ph, sh = reads[kh]
                    first = jnp.concatenate([planes[ph, sh, q, kt] for q in range(4)], axis=0)
                    second = jnp.concatenate([planes[ph, sh, q + 1, kt] for q in range(4)], axis=0)
                    k0, k1, k2 = (wf[kt, kh, kw] for kw in range(3))
                    if b == 0:
                        cols += [first, second[:, 128:]]
                        rhs += [k1, k0, zero, k2]
                    else:
                        cols += [first[:, :256], second]
                        rhs += [k0, zero, k2, k1]
            d = dot(jnp.concatenate(cols, axis=1), jnp.concatenate(rhs, axis=0))
            for q in range(4):
                l = jnp.concatenate([dense(lift.at[a, q + b, b + c], a, 2) for c in range(2)], axis=1)
                v = d[48 * q:48 * q + 48] + ((l[:, 64:] if b else l[:, :c1]) + b2)
                back[a, 0, pl.ds(2 * q + b, 48, stride=8), :] = v[:, :128]
                back[a, 1, pl.ds(2 * q + b, 48, stride=8), 0:64] = v[:, 128:]
        for t in range(4):
            for i in range(12):
                at = 96 * t + 8 * i
                out[t, 2 * i + a] = jnp.concatenate([back[a, 0, at:at + 8, :], back[a, 1, at:at + 8, 0:64]], axis=1).astype(BF)


def block(x, gain0, wc, bias0, wu, bias1, gain1, wf, bias2, *, nt, ns):
    c0, c1 = wc.shape[-1], wf.shape[-1]
    at = lambda t, s: t * ns + s
    vm = pl.BlockSpec(memory_space=pltpu.VMEM)
    hbm = pl.BlockSpec(memory_space=pltpu.HBM)
    far = lambda v: pltpu.with_memory_space_constraint(v, pltpu.HBM)
    two = lambda v: v.reshape(1, -1)
    axes = ("tm", "strip")
    prev = lax.ppermute(x, axes, [(at(t, s), at(t + 1, s)) for t in range(nt - 1) for s in range(ns)])
    w4, wv, part = pl.pallas_call(
        own,
        out_shape=(jax.ShapeDtypeStruct((4 * c0, 4 * c1), BF), jax.ShapeDtypeStruct(wc.shape, BF),
                   jax.ShapeDtypeStruct((256, c0), F32)),
        in_specs=[hbm] * 4,
        out_specs=(vm, vm, vm),
        scratch_shapes=[
            pltpu.VMEM(x.shape, BF),
            pltpu.VMEM((c0,), F32),
            pltpu.VMEM((3, 3, c1, c0), BF),
            pltpu.VMEM((4 * c1, 4 * c0), BF),
            pltpu.VMEM((3, 272, 128), F32),
            pltpu.VMEM((3, 256, c0), BF),
            pltpu.SemaphoreType.DMA((6,)),
        ],
        compiler_params=pltpu.CompilerParams(vmem_limit_bytes=26 << 20),
    )(far(x), far(gain0), far(wc), far(jnp.swapaxes(wu, 2, 3)))
    both = jnp.concatenate([prev, x], axis=0)
    odd = lax.axis_index("strip") % 2 == 1
    top, bottom = both[:, :2], both[:, 10:]
    inner = lax.ppermute(jnp.where(odd, top, bottom), axes,
                         [(at(t, s), at(t, s ^ 1)) for t in range(nt) for s in range(ns)])
    outer = lax.ppermute(jnp.where(odd, bottom, top), axes,
                         [(at(t, s), at(t, s + 1 if s % 2 else s - 1)) for t in range(nt) for s in range(1, ns - 1)])
    sums = pl.pallas_call(
        old,
        out_shape=jax.ShapeDtypeStruct((384, c0), F32),
        in_specs=[vm] * 5,
        out_specs=vm,
        scratch_shapes=[pltpu.VMEM((3, 272, 128), F32), pltpu.VMEM((3, 256, c0), BF)],
        compiler_params=pltpu.CompilerParams(vmem_limit_bytes=14 << 20),
    )(part, prev, gain0, wv, bias0)
    return pl.pallas_call(
        functools.partial(kernel, ns - 1),
        out_shape=jax.ShapeDtypeStruct((4, 24, 8, c1), BF),
        in_specs=[vm] * 10,
        out_specs=vm,
        scratch_shapes=[
            pltpu.VMEM((3, 128, 128), F32),
            pltpu.VMEM((2, 384, c0), BF),
            pltpu.VMEM((3, 3, 128, c0), BF),
            pltpu.VMEM((3, 128, 128), F32),
            pltpu.VMEM((3, 400, 128), F32),
            pltpu.VMEM((2, 5, 3, 112, 128), F32),
            pltpu.VMEM((2, 5, 3, 112, 128), F32),
            pltpu.VMEM((2, 2, 5, 3, 48, 2 * c1), BF),
            pltpu.VMEM((2, 2, 384, 128), F32),
        ],
        compiler_params=pltpu.CompilerParams(vmem_limit_bytes=14 << 20),
    )(sums, inner, outer, gain0, wv, w4, two(bias1), two(gain1), wf, two(bias2))


def solution(mesh):
    nt, ns = mesh.shape["tm"], mesh.shape["strip"]
    part = P("tm", "strip", None, None)
    return jax.shard_map(
        functools.partial(block, nt=nt, ns=ns), mesh=mesh,
        in_specs=(part,) + (P(),) * 8, out_specs=part, check_vma=False)
```

```python
import functools

import jax
import jax.numpy as jnp
from jax import lax
from jax.experimental import pallas as pl
from jax.experimental.pallas import tpu as pltpu
from jax.sharding import PartitionSpec as P


EPS = 1e-6
BF = jnp.bfloat16
F32 = jnp.float32


def silu(v):
    half = 0.5 * v
    return half + half * jnp.tanh(half)


def dot(a, b):
    return jnp.dot(a, b, preferred_element_type=F32)


def phases(wu, w4, turned):
    c1, c0 = wu.shape[2:]
    for r in range(0, c1, 16):
        f = [[wu[kh, kw, r:r + 16, :].astype(F32) for kw in range(3)] for kh in range(3)]
        cols = [[(k[0], k[1] + k[2]), (k[0] + k[1], k[2])] for k in f]
        for wcol in range(2):
            tap = [[cols[kh][b][wcol] for b in range(2)] for kh in range(3)]
            first = tap[0] + [tap[0][b] + tap[1][b] for b in range(2)]
            second = [tap[1][b] + tap[2][b] for b in range(2)] + tap[2]
            for hrow, parts in enumerate((first, second)):
                at = (2 * wcol + hrow) * c0
                for i, v in enumerate(parts):
                    turned[c1 * i + r:c1 * i + r + 16, at:at + c0] = v.astype(BF)
    for k in range(0, 4 * c0, 128):
        w4[k:k + 128, :] = turned[:, k:k + 128].T


def put(raw, row, v):
    for c in range(3):
        raw[c, row:row + v.shape[0], :] = v[:, 128 * c:128 * c + 128]


def normed(raw, row, g0):
    v = jnp.concatenate([raw[c, row:row + 64, :] for c in range(3)], axis=1)
    r = lax.rsqrt(jnp.mean(v * v, axis=-1, keepdims=True) + EPS)
    return silu(v * r * g0)


def spread(raw, left, t):
    for kh in range(3):
        for w in range(4):
            for c in range(3):
                v = raw[c, pl.ds(64 * t + 4 * kh + w, 16, stride=4), :]
                left[kh, 64 * t + 16 * w:64 * t + 16 * w + 16, 128 * c:128 * c + 128] = v.astype(BF)


SPAN = ((0, 3), (0, 4), (1, 3))


def blank(raw, n):
    zero = jnp.zeros((8, 3 * raw.shape[-1]), F32)
    for t in range(n):
        put(raw, 64 * t, zero)
        put(raw, 64 * t + 56, zero)
    put(raw, 64 * n, zero)


def gather(left, lo, m, first, n):
    return jnp.concatenate(
        [jnp.concatenate([left[kh, 64 * t + 16 * lo:64 * t + 16 * (lo + m), :] for t in range(first, first + n)], axis=0)
         for kh in range(3)], axis=1)


def stack(wc, kt, kw):
    return jnp.concatenate([wc[kt, kh, kw] for kh in range(3)], axis=0)


def own(x_hbm, gain0_hbm, wc, wu_hbm, w4, wv, part, x, gain0, wu, turned, raw, left, sems):
    c0 = x.shape[-1]
    get_x = pltpu.make_async_copy(x_hbm, x, sems.at[3])
    get_x.start()
    get_g = pltpu.make_async_copy(gain0_hbm, gain0, sems.at[5])
    get_g.start()
    get_u = pltpu.make_async_copy(wu_hbm, wu, sems.at[4])
    get_u.start()
    copies = {}
    for kt in (2, 1, 0):
        copies[kt] = pltpu.make_async_copy(wc.at[kt], wv.at[kt], sems.at[kt])
        copies[kt].start()
    blank(raw, 4)
    get_x.wait()
    get_g.wait()
    g0 = gain0[...].reshape(1, c0)
    for t in range(4):
        for h in range(12):
            put(raw, 64 * t + 8 + 4 * h, x[t, h].astype(F32))
        put(raw, 64 * t, normed(raw, 64 * t, g0))
    for t in range(4):
        spread(raw, left, t)
    get_u.wait()
    phases(wu, w4, turned)
    for kt in (2, 1, 0):
        copies[kt].wait()
        n = kt + 2
        for kw in (1, 0, 2):
            lo, m = SPAN[kw]
            d = dot(gather(left, lo, m, 0, n), stack(wv, kt, kw))
            for t in range(n):
                at = 64 * (t + 2 - kt) + 16 * (lo + 1 - kw)
                v = d[16 * m * t:16 * m * (t + 1)]
                if kt == 2 and kw == 1:
                    part[at:at + 16 * m, :] = v
                else:
                    part[at:at + 16 * m, :] += v


def old(part, prev, gain0, wc, bias0, mid, raw, left):
    c0 = prev.shape[-1]
    g0 = gain0[...].reshape(1, c0)
    b0 = bias0[...].reshape(1, c0)
    blank(raw, 4)
    for t in range(4):
        for h in range(12):
            put(raw, 64 * t + 8 + 4 * h, prev[t, h].astype(F32))
        put(raw, 64 * t, normed(raw, 64 * t, g0))
    for t in range(4):
        spread(raw, left, t)
    mid[0:128, :] = jnp.broadcast_to(b0, (128, c0))
    mid[128:384, :] = part[...] + b0
    for kt in range(3):
        n = 4 - kt
        for kw in range(3):
            lo, m = SPAN[kw]
            d = dot(gather(left, lo, m, kt, n), stack(wc, kt, kw))
            for u in range(n):
                at = 64 * u + 16 * (lo + 1 - kw)
                mid[at:at + 16 * m, :] += d[16 * m * u:16 * m * (u + 1)]


def kernel(last, sums, inner, outer, gain0, wc, w4, bias1, gain1, wf, bias2, out,
           raw, left, ends, tail, mid, lift, lines, planes, back):
    group = lax.axis_index("tm")
    strip = lax.axis_index("strip")
    c0 = wc.shape[-1]
    c1 = wf.shape[-1]
    odd = strip % 2 == 1

    sub = lax.broadcasted_iota(jnp.int32, (8, 128), 0)

    @pl.when(strip >= 0)
    def _():
        for t in range(8):
            for i in range(2):
                a, b = inner[t, i].astype(F32), outer[t, i].astype(F32)
                put(raw, 16 * t + 4 * i, jnp.where(odd, a, b))
                put(raw, 16 * t + 8 + 4 * i, jnp.where(odd, b, a))
        g0 = gain0[...].reshape(1, c0)
        row = lax.broadcasted_iota(jnp.int32, (8, c0), 0)
        none = jnp.zeros((8, c0), F32)
        for half in range(2):
            v = normed(raw, 64 * half, g0)
            for i in range(4):
                t = 4 * half + i
                up, down = v[16 * i:16 * i + 8], v[16 * i + 8:16 * i + 16]
                for kh in range(3):
                    a = (up, jnp.where(row < 4, pltpu.roll(up, 4, 0), 0.0), none)[kh]
                    b = (none, jnp.where(row < 4, 0.0, pltpu.roll(down, 4, 0)), down)[kh]
                    for kw in range(3):
                        if kw == 0:
                            e = [jnp.where(row % 4 == 0, 0.0, pltpu.roll(z, 1, 0)) for z in (a, b)]
                        elif kw == 2:
                            e = [jnp.where(row % 4 == 3, 0.0, pltpu.roll(z, 7, 0)) for z in (a, b)]
                        else:
                            e = [a, b]
                        ends[kw, kh, 16 * t:16 * t + 16, :] = jnp.concatenate(e, axis=0).astype(BF)
        every = [(kt, kw, kh) for kt in range(3) for kw in range(3) for kh in range(3)]
        d = dot(jnp.concatenate([ends[kw, kh, 16 * kt:16 * kt + 96, :] for kt, kw, kh in every], axis=1),
                jnp.concatenate([wc[kt, kh, kw] for kt, kw, kh in every], axis=0))
        for c in range(3):
            tail[c, 8:104, :] = d[:, 128 * c:128 * c + 128]
        keep_top = jnp.logical_or(strip > 0, sub != 0)
        keep_end = jnp.logical_or(strip < last, sub != 5)
        for t in range(6):
            for w in range(4):
                at = 64 * t + 16 * w
                for c in range(3):
                    lanes = slice(128 * c, 128 * c + 128)
                    top = sums[at:at + 8, lanes] + jnp.where(sub < 2, tail[c, pl.ds(16 * t + w + 8, 8, stride=4), :], 0.0)
                    add = jnp.where(sub // 2 == 2, tail[c, pl.ds(16 * t + w, 8, stride=4), :], 0.0)
                    end = sums[at + 8:at + 16, lanes] + add
                    v = jnp.concatenate([jnp.where(keep_top, top, 0.0), jnp.where(keep_end, end, 0.0)], axis=0)
                    mid[c, at:at + 16, :] = v
                    left[0, at:at + 16, lanes] = v.astype(BF)
        for at in range(0, 384, 16):
            for c in range(3):
                left[1, at:at + 16, 128 * c:128 * c + 128] = mid[c, at + 1:at + 17, :].astype(BF)

    def ups(lo, n, first, count):
        both = [jnp.concatenate([left[i, 64 * t + 16 * lo:64 * t + 16 * (lo + n), :] for t in range(first, first + count)],
                                axis=0) for i in range(2)]
        return jnp.concatenate(both, axis=1)

    def thirds(v):
        v = jnp.concatenate([v, v], axis=1)
        return [v[:, 128 * c:128 * c + 128] for c in range(3)]

    b1 = thirds(bias1[...])
    g1 = thirds(0.5 * gain1[...])
    low = lax.broadcasted_iota(jnp.int32, (16, 128), 1) < 64
    row = lax.broadcasted_iota(jnp.int32, (16, 1), 0)
    ok_end = jnp.logical_or(strip < last, row != 12)
    ok_top = jnp.logical_or(strip > 0, row != 0)
    early = [jnp.logical_and(ok, group > 0) for ok in (ok_end, ok_top)]

    def finish(u, p, t, a):
        l = [None if u[c] is None else (u[c] + b1[c]).astype(BF).astype(F32) for c in range(3)]
        at = 16 * t
        for c in range(3):
            if l[c] is not None:
                lift[a, p, c, at:at + 16, :] = l[c]
        ok = early[a] if t < 2 else (ok_end, ok_top)[a]
        mids = l[1] * l[1]
        part = jnp.where(low, mids, 0.0)
        re = ro = jnp.zeros((16, 1), F32)
        if p < 4:
            re = jnp.sum(l[0] * l[0] + part, axis=-1, keepdims=True) * (1.0 / c1)
            re = jnp.where(ok, lax.rsqrt(re + EPS), 0.0)
        if p > 0:
            ro = jnp.sum(l[2] * l[2] + (mids - part), axis=-1, keepdims=True) * (1.0 / c1)
            ro = jnp.where(ok, lax.rsqrt(ro + EPS), 0.0)
        for c, r in enumerate((re, jnp.where(low, re, ro), ro)):
            if l[c] is not None:
                h = l[c] * (r * g1[c])
                lines[a, p, c, at:at + 16, :] = h + h * jnp.tanh(h)

    def dense(ref, s, kt):
        rows = lambda t, k: ref[16 * t + s + k:16 * t + s + k + 8, :]
        seam = lambda t: jnp.where(sub < 4, rows(t, 8), rows(t + 1, -4))
        return jnp.concatenate(
            [rows(kt, 0), seam(kt), rows(kt + 1, 4), rows(kt + 2, 0), seam(kt + 2), rows(kt + 3, 4)], axis=0)

    def pack(p, kts=range(3)):
        for kt in kts:
            for a in range(2):
                for s in range(2):
                    for c in range(3):
                        none = p == 0 and c == 2 or p == 4 and c == 0
                        v = jnp.zeros((48, 128), BF) if none else dense(lines.at[a, p, c], s, kt).astype(BF)
                        planes[a, s, p, kt, :, 128 * c:128 * c + 128] = v

    def edge(p):
        lhs, rhs = (ups(0, 1, 0, 6), slice(2 * c0, 4 * c0)) if p == 0 else (ups(3, 1, 0, 6), slice(0, 2 * c0))
        u = []
        for a in range(2):
            n = 2 * c1 * a + (0 if p == 0 else 128)
            d = dot(lhs, w4[rhs, n:n + 256])
            u.append([d[:, :128], d[:, 128:], None] if p == 0 else [None, d[:, :128], d[:, 128:]])
        return u

    def chunk(first, count):
        return dot(jnp.concatenate([ups(0, 3, first, count), ups(1, 3, first, count)], axis=1), w4[...])

    def finish_edge(u, p):
        for t in range(6):
            for a in range(2):
                finish([v if v is None else v[16 * t:16 * t + 16] for v in u[a]], p, t, a)
        pack(p)

    def finish_chunk(u, first, count):
        for t in range(count):
            for p in range(1, 4):
                at = 48 * t + 16 * (p - 1)
                for a in range(2):
                    n = 2 * c1 * a
                    finish([u[at:at + 16, n + 128 * c:n + 128 * c + 128] for c in range(3)], p, first + t, a)

    ua = chunk(0, 4)
    u0, u4 = edge(0), edge(4)
    finish_chunk(ua, 0, 4)
    ub = chunk(4, 2)
    for p in range(1, 4):
        pack(p, (0,))
    finish_edge(u0, 0)
    finish_edge(u4, 4)
    finish_chunk(ub, 4, 2)
    for p in range(1, 4):
        pack(p, (1, 2))
    b2 = bias2[...]
    zero = jnp.zeros((64, c1), BF)
    for a in range(2):
        reads = ((1, 0), (0, 0), (1, 1)) if a == 0 else ((0, 0), (1, 1), (0, 1))
        for b in (1, 0):
            cols, rhs, half = [], [], []
            for kt in range(3):
                for kh in range(3):
                    ph, sh = reads[kh]
                    first = jnp.concatenate([planes[ph, sh, q, kt] for q in range(4)], axis=0)
                    second = jnp.concatenate([planes[ph, sh, q + 1, kt] for q in range(4)], axis=0)
                    k0, k1, k2 = (wf.at[kt, kh, kw] for kw in range(3))
                    if b == 0:
                        cols += [first, second[:, 256:]]
                        rhs += [k1[...], k0[...], k2[64:, :]]
                        half.append((second[:, 192:256], k2[0:64, :]))
                    else:
                        cols += [first[:, :128], second]
                        rhs += [k0[0:128, :], k2[...], k1[...]]
                        half.append((first[:, 128:192], k0[128:, :]))
            for i in range(0, 9, 2):
                pair = half[i:i + 2] if i < 8 else [half[8], (half[8][0], zero)]
                cols.append(jnp.concatenate([v for v, _ in pair], axis=1))
                rhs += [k for _, k in pair]
            d = dot(jnp.concatenate(cols, axis=1), jnp.concatenate(rhs, axis=0))
            for q in range(4):
                l = jnp.concatenate([dense(lift.at[a, q + b, b + c], a, 2) for c in range(2)], axis=1)
                v = d[48 * q:48 * q + 48] + ((l[:, 64:] if b else l[:, :c1]) + b2)
                back[a, 0, pl.ds(2 * q + b, 48, stride=8), :] = v[:, :128]
                back[a, 1, pl.ds(2 * q + b, 48, stride=8), 0:64] = v[:, 128:]
        for t in range(4):
            for i in range(12):
                at = 96 * t + 8 * i
                out[t, 2 * i + a] = jnp.concatenate([back[a, 0, at:at + 8, :], back[a, 1, at:at + 8, 0:64]], axis=1).astype(BF)


def block(x, gain0, wc, bias0, wu, bias1, gain1, wf, bias2, *, nt, ns):
    c0, c1 = wc.shape[-1], wf.shape[-1]
    at = lambda t, s: t * ns + s
    vm = pl.BlockSpec(memory_space=pltpu.VMEM)
    hbm = pl.BlockSpec(memory_space=pltpu.HBM)
    far = lambda v: pltpu.with_memory_space_constraint(v, pltpu.HBM)
    two = lambda v: v.reshape(1, -1)
    axes = ("tm", "strip")
    prev = lax.ppermute(x, axes, [(at(t, s), at(t + 1, s)) for t in range(nt - 1) for s in range(ns)])
    w4, wv, part = pl.pallas_call(
        own,
        out_shape=(jax.ShapeDtypeStruct((4 * c0, 4 * c1), BF), jax.ShapeDtypeStruct(wc.shape, BF),
                   jax.ShapeDtypeStruct((256, c0), F32)),
        in_specs=[hbm] * 4,
        out_specs=(vm, vm, vm),
        scratch_shapes=[
            pltpu.VMEM(x.shape, BF),
            pltpu.VMEM((c0,), F32),
            pltpu.VMEM((3, 3, c1, c0), BF),
            pltpu.VMEM((4 * c1, 4 * c0), BF),
            pltpu.VMEM((3, 272, 128), F32),
            pltpu.VMEM((3, 256, c0), BF),
            pltpu.SemaphoreType.DMA((6,)),
        ],
        compiler_params=pltpu.CompilerParams(vmem_limit_bytes=26 << 20),
    )(far(x), far(gain0), far(wc), far(jnp.swapaxes(wu, 2, 3)))
    odd = lax.axis_index("strip") % 2 == 1
    top, bottom = (jnp.concatenate([v[:, rows] for v in (prev, x)], axis=0) for rows in (slice(0, 2), slice(10, 12)))
    inner = lax.ppermute(jnp.where(odd, top, bottom), axes,
                         [(at(t, s), at(t, s ^ 1)) for t in range(nt) for s in range(ns)])
    outer = lax.ppermute(jnp.where(odd, bottom, top), axes,
                         [(at(t, s), at(t, s + 1 if s % 2 else s - 1)) for t in range(nt) for s in range(1, ns - 1)])
    sums = pl.pallas_call(
        old,
        out_shape=jax.ShapeDtypeStruct((384, c0), F32),
        in_specs=[vm] * 5,
        out_specs=vm,
        scratch_shapes=[pltpu.VMEM((3, 272, 128), F32), pltpu.VMEM((3, 256, c0), BF)],
        compiler_params=pltpu.CompilerParams(vmem_limit_bytes=14 << 20),
    )(part, prev, gain0, wv, bias0)
    return pl.pallas_call(
        functools.partial(kernel, ns - 1),
        out_shape=jax.ShapeDtypeStruct((4, 24, 8, c1), BF),
        in_specs=[vm] * 10,
        out_specs=vm,
        scratch_shapes=[
            pltpu.VMEM((3, 128, 128), F32),
            pltpu.VMEM((2, 384, c0), BF),
            pltpu.VMEM((3, 3, 128, c0), BF),
            pltpu.VMEM((3, 128, 128), F32),
            pltpu.VMEM((3, 400, 128), F32),
            pltpu.VMEM((2, 5, 3, 112, 128), F32),
            pltpu.VMEM((2, 5, 3, 112, 128), F32),
            pltpu.VMEM((2, 2, 5, 3, 48, 2 * c1), BF),
            pltpu.VMEM((2, 2, 384, 128), F32),
        ],
        compiler_params=pltpu.CompilerParams(vmem_limit_bytes=14 << 20),
    )(sums, inner, outer, gain0, wv, w4, two(bias1), two(gain1), wf, two(bias2))


def solution(mesh):
    nt, ns = mesh.shape["tm"], mesh.shape["strip"]
    part = P("tm", "strip", None, None)
    return jax.shard_map(
        functools.partial(block, nt=nt, ns=ns), mesh=mesh,
        in_specs=(part,) + (P(),) * 8, out_specs=part, check_vma=False)
```

```python
import functools

import jax
import jax.numpy as jnp
from jax import lax
from jax.experimental import pallas as pl
from jax.experimental.pallas import tpu as pltpu
from jax.sharding import PartitionSpec as P


EPS = 1e-6
BF = jnp.bfloat16
F32 = jnp.float32


def silu(v):
    half = 0.5 * v
    return half + half * jnp.tanh(half)


def dot(a, b):
    return jnp.dot(a, b, preferred_element_type=F32)


def phases(wu, w4, turned):
    c1, c0 = wu.shape[2:]
    for r in range(0, c1, 16):
        f = [[wu[kh, kw, r:r + 16, :].astype(F32) for kw in range(3)] for kh in range(3)]
        cols = [[(k[0], k[1] + k[2]), (k[0] + k[1], k[2])] for k in f]
        for wcol in range(2):
            tap = [[cols[kh][b][wcol] for b in range(2)] for kh in range(3)]
            first = tap[0] + [tap[0][b] + tap[1][b] for b in range(2)]
            second = [tap[1][b] + tap[2][b] for b in range(2)] + tap[2]
            for hrow, parts in enumerate((first, second)):
                at = (2 * wcol + hrow) * c0
                for i, v in enumerate(parts):
                    turned[c1 * i + r:c1 * i + r + 16, at:at + c0] = v.astype(BF)
    for k in range(0, 4 * c0, 128):
        w4[k:k + 128, :] = turned[:, k:k + 128].T


def put(raw, row, v):
    for c in range(3):
        raw[c, row:row + v.shape[0], :] = v[:, 128 * c:128 * c + 128]


def normed(raw, row, g0):
    v = jnp.concatenate([raw[c, row:row + 64, :] for c in range(3)], axis=1)
    r = lax.rsqrt(jnp.mean(v * v, axis=-1, keepdims=True) + EPS)
    return silu(v * r * g0)


def spread(raw, left, t):
    for kh in range(3):
        for w in range(4):
            for c in range(3):
                v = raw[c, pl.ds(64 * t + 4 * kh + w, 16, stride=4), :]
                left[kh, 64 * t + 16 * w:64 * t + 16 * w + 16, 128 * c:128 * c + 128] = v.astype(BF)


SPAN = ((0, 3), (0, 4), (1, 3))


def blank(raw, n):
    zero = jnp.zeros((8, 3 * raw.shape[-1]), F32)
    for t in range(n):
        put(raw, 64 * t, zero)
        put(raw, 64 * t + 56, zero)
    put(raw, 64 * n, zero)


def gather(left, lo, m, first, n):
    return jnp.concatenate(
        [jnp.concatenate([left[kh, 64 * t + 16 * lo:64 * t + 16 * (lo + m), :] for t in range(first, first + n)], axis=0)
         for kh in range(3)], axis=1)


def stack(wc, kt, kw):
    return jnp.concatenate([wc[kt, kh, kw] for kh in range(3)], axis=0)


def own(x_hbm, gain0_hbm, wc, wu_hbm, w4, wv, part, mine, x, gain0, wu, turned, raw, left, sems):
    c0 = x.shape[-1]
    get_x = pltpu.make_async_copy(x_hbm, x, sems.at[3])
    get_x.start()
    get_g = pltpu.make_async_copy(gain0_hbm, gain0, sems.at[5])
    get_g.start()
    get_u = pltpu.make_async_copy(wu_hbm, wu, sems.at[4])
    get_u.start()
    copies = {}
    for kt in (2, 1, 0):
        copies[kt] = pltpu.make_async_copy(wc.at[kt], wv.at[kt], sems.at[kt])
        copies[kt].start()
    blank(raw, 4)
    get_x.wait()
    mine[0] = x[:, :2]
    mine[1] = x[:, 10:]
    get_g.wait()
    g0 = gain0[...].reshape(1, c0)
    for t in range(4):
        for h in range(12):
            put(raw, 64 * t + 8 + 4 * h, x[t, h].astype(F32))
        put(raw, 64 * t, normed(raw, 64 * t, g0))
    for t in range(4):
        spread(raw, left, t)
    get_u.wait()
    phases(wu, w4, turned)
    for kt in (2, 1, 0):
        copies[kt].wait()
        n = kt + 2
        for kw in (1, 0, 2):
            lo, m = SPAN[kw]
            d = dot(gather(left, lo, m, 0, n), stack(wv, kt, kw))
            for t in range(n):
                at = 64 * (t + 2 - kt) + 16 * (lo + 1 - kw)
                v = d[16 * m * t:16 * m * (t + 1)]
                if kt == 2 and kw == 1:
                    part[at:at + 16 * m, :] = v
                else:
                    part[at:at + 16 * m, :] += v


def shares(wc, mid, left, kts):
    for kt in kts:
        n = 4 - kt
        for kw in range(3):
            lo, m = SPAN[kw]
            d = dot(gather(left, lo, m, kt, n), stack(wc, kt, kw))
            for u in range(n):
                at = 64 * u + 16 * (lo + 1 - kw)
                mid[at:at + 16 * m, :] += d[16 * m * u:16 * m * (u + 1)]


def begin(part, prev, gain0, wc, bias0, mid, left, raw):
    c0 = prev.shape[-1]
    g0 = gain0[...].reshape(1, c0)
    b0 = bias0[...].reshape(1, c0)
    blank(raw, 4)
    for t in range(4):
        for h in range(12):
            put(raw, 64 * t + 8 + 4 * h, prev[t, h].astype(F32))
        put(raw, 64 * t, normed(raw, 64 * t, g0))
    for t in range(4):
        spread(raw, left, t)
    mid[0:128, :] = jnp.broadcast_to(b0, (128, c0))
    mid[128:384, :] = part[...] + b0
    shares(wc, mid, left, (0,))


def early(part, prev, mine, gain0, wc, bias0, inner, outer, mid, left, raw):
    odd = lax.axis_index("strip") % 2 == 1

    @pl.when(odd)
    def _():
        inner[0:4], inner[4:8] = prev[:, :2], mine[0]
        outer[0:4], outer[4:8] = prev[:, 10:], mine[1]
        begin(part, prev, gain0, wc, bias0, mid, left, raw)

    @pl.when(jnp.logical_not(odd))
    def _():
        inner[0:4], inner[4:8] = prev[:, 10:], mine[1]
        outer[0:4], outer[4:8] = prev[:, :2], mine[0]


def old(part, prev, gain0, wc, bias0, mid_in, left_in, mid, left, raw):
    @pl.when(lax.axis_index("strip") % 2 == 0)
    def _():
        begin(part, prev, gain0, wc, bias0, mid, left, raw)

    shares(wc, mid, left, (1, 2))


def kernel(last, sums, inner, outer, gain0, wc, w4, bias1, gain1, wf, bias2, out,
           raw, left, ends, tail, mid, lift, lines, planes, back):
    group = lax.axis_index("tm")
    strip = lax.axis_index("strip")
    c0 = wc.shape[-1]
    c1 = wf.shape[-1]
    odd = strip % 2 == 1

    sub = lax.broadcasted_iota(jnp.int32, (8, 128), 0)

    @pl.when(strip >= 0)
    def _():
        for t in range(8):
            for i in range(2):
                a, b = inner[t, i].astype(F32), outer[t, i].astype(F32)
                put(raw, 16 * t + 4 * i, jnp.where(odd, a, b))
                put(raw, 16 * t + 8 + 4 * i, jnp.where(odd, b, a))
        g0 = gain0[...].reshape(1, c0)
        row = lax.broadcasted_iota(jnp.int32, (8, c0), 0)
        none = jnp.zeros((8, c0), F32)
        v = [normed(raw, 64 * half, g0) for half in range(2)]
        up = [v[t // 4][16 * (t % 4):16 * (t % 4) + 8] for t in range(8)]
        down = [v[t // 4][16 * (t % 4) + 8:16 * (t % 4) + 16] for t in range(8)]

        def end(kw, kh, t):
            a = (up[t], jnp.where(row < 4, pltpu.roll(up[t], 4, 0), 0.0), none)[kh]
            b = (none, jnp.where(row < 4, 0.0, pltpu.roll(down[t], 4, 0)), down[t])[kh]
            if kw == 0:
                e = [jnp.where(row % 4 == 0, 0.0, pltpu.roll(z, 1, 0)) for z in (a, b)]
            elif kw == 2:
                e = [jnp.where(row % 4 == 3, 0.0, pltpu.roll(z, 7, 0)) for z in (a, b)]
            else:
                e = [a, b]
            return jnp.concatenate(e, axis=0).astype(BF)

        every = [(kt, kw, kh) for kw, kh in ((1, 0), (1, 2), (1, 1), (0, 0), (0, 2), (0, 1), (2, 0), (2, 2), (2, 1))
                 for kt in range(3)]
        for kt, kw, kh in every:
            if kt == 0:
                for t in range(8):
                    ends[kw, kh, 16 * t:16 * t + 16, :] = end(kw, kh, t)
        d = dot(jnp.concatenate([ends[kw, kh, 16 * kt:16 * kt + 96, :] for kt, kw, kh in every], axis=1),
                jnp.concatenate([wc[kt, kh, kw] for kt, kw, kh in every], axis=0))
        for c in range(3):
            tail[c, 8:104, :] = d[:, 128 * c:128 * c + 128]
        keep_top = jnp.logical_or(strip > 0, sub != 0)
        keep_end = jnp.logical_or(strip < last, sub != 5)
        for t in range(6):
            for w in range(4):
                at = 64 * t + 16 * w
                for c in range(3):
                    lanes = slice(128 * c, 128 * c + 128)
                    top = sums[at:at + 8, lanes] + jnp.where(sub < 2, tail[c, pl.ds(16 * t + w + 8, 8, stride=4), :], 0.0)
                    add = jnp.where(sub // 2 == 2, tail[c, pl.ds(16 * t + w, 8, stride=4), :], 0.0)
                    end = sums[at + 8:at + 16, lanes] + add
                    v = jnp.concatenate([jnp.where(keep_top, top, 0.0), jnp.where(keep_end, end, 0.0)], axis=0)
                    mid[c, at:at + 16, :] = v
                    left[0, at:at + 16, lanes] = v.astype(BF)
        for at in range(0, 384, 16):
            for c in range(3):
                left[1, at:at + 16, 128 * c:128 * c + 128] = mid[c, at + 1:at + 17, :].astype(BF)

    def ups(lo, n, first, count):
        both = [jnp.concatenate([left[i, 64 * t + 16 * lo:64 * t + 16 * (lo + n), :] for t in range(first, first + count)],
                                axis=0) for i in range(2)]
        return jnp.concatenate(both, axis=1)

    def thirds(v):
        v = jnp.concatenate([v, v], axis=1)
        return [v[:, 128 * c:128 * c + 128] for c in range(3)]

    b1 = thirds(bias1[...])
    g1 = thirds(0.5 * gain1[...])
    low = lax.broadcasted_iota(jnp.int32, (16, 128), 1) < 64
    row = lax.broadcasted_iota(jnp.int32, (16, 1), 0)
    ok_end = jnp.logical_or(strip < last, row != 12)
    ok_top = jnp.logical_or(strip > 0, row != 0)
    early = [jnp.logical_and(ok, group > 0) for ok in (ok_end, ok_top)]

    def finish(u, p, t, a):
        l = [None if u[c] is None else (u[c] + b1[c]).astype(BF).astype(F32) for c in range(3)]
        at = 16 * t
        for c in range(3):
            if l[c] is not None:
                lift[a, p, c, at:at + 16, :] = l[c]
        ok = early[a] if t < 2 else (ok_end, ok_top)[a]
        mids = l[1] * l[1]
        part = jnp.where(low, mids, 0.0)
        re = ro = jnp.zeros((16, 1), F32)
        if p < 4:
            re = jnp.sum(l[0] * l[0] + part, axis=-1, keepdims=True) * (1.0 / c1)
            re = jnp.where(ok, lax.rsqrt(re + EPS), 0.0)
        if p > 0:
            ro = jnp.sum(l[2] * l[2] + (mids - part), axis=-1, keepdims=True) * (1.0 / c1)
            ro = jnp.where(ok, lax.rsqrt(ro + EPS), 0.0)
        for c, r in enumerate((re, jnp.where(low, re, ro), ro)):
            if l[c] is not None:
                h = l[c] * (r * g1[c])
                lines[a, p, c, at:at + 16, :] = h + h * jnp.tanh(h)

    def dense(ref, s, kt):
        rows = lambda t, k: ref[16 * t + s + k:16 * t + s + k + 8, :]
        seam = lambda t: jnp.where(sub < 4, rows(t, 8), rows(t + 1, -4))
        return jnp.concatenate(
            [rows(kt, 0), seam(kt), rows(kt + 1, 4), rows(kt + 2, 0), seam(kt + 2), rows(kt + 3, 4)], axis=0)

    def pack(p, kts=range(3)):
        for kt in kts:
            for a in range(2):
                for s in range(2):
                    for c in range(3):
                        none = p == 0 and c == 2 or p == 4 and c == 0
                        v = jnp.zeros((48, 128), BF) if none else dense(lines.at[a, p, c], s, kt).astype(BF)
                        planes[a, s, p, kt, :, 128 * c:128 * c + 128] = v

    def edge(p):
        lhs, rhs = (ups(0, 1, 0, 6), slice(2 * c0, 4 * c0)) if p == 0 else (ups(3, 1, 0, 6), slice(0, 2 * c0))
        u = []
        for a in range(2):
            n = 2 * c1 * a + (0 if p == 0 else 128)
            d = dot(lhs, w4[rhs, n:n + 256])
            u.append([d[:, :128], d[:, 128:], None] if p == 0 else [None, d[:, :128], d[:, 128:]])
        return u

    def chunk(first, count):
        return dot(jnp.concatenate([ups(0, 3, first, count), ups(1, 3, first, count)], axis=1), w4[...])

    def finish_edge(u, p):
        for t in range(6):
            for a in range(2):
                finish([v if v is None else v[16 * t:16 * t + 16] for v in u[a]], p, t, a)
        pack(p)

    def finish_chunk(u, first, count):
        for t in range(count):
            for p in range(1, 4):
                at = 48 * t + 16 * (p - 1)
                for a in range(2):
                    n = 2 * c1 * a
                    finish([u[at:at + 16, n + 128 * c:n + 128 * c + 128] for c in range(3)], p, first + t, a)

    ua = chunk(0, 4)
    u0, u4 = edge(0), edge(4)
    finish_chunk(ua, 0, 4)
    ub = chunk(4, 2)
    for p in range(1, 4):
        pack(p, (0,))
    finish_edge(u0, 0)
    finish_edge(u4, 4)
    finish_chunk(ub, 4, 2)
    for p in range(1, 4):
        pack(p, (1, 2))
    b2 = bias2[...]
    zero = jnp.zeros((64, c1), BF)
    for a in range(2):
        reads = ((1, 0), (0, 0), (1, 1)) if a == 0 else ((0, 0), (1, 1), (0, 1))
        for b in (1, 0):
            cols, rhs = [], []
            for kt in range(3):
                for kh in range(3):
                    ph, sh = reads[kh]
                    first = jnp.concatenate([planes[ph, sh, q, kt] for q in range(4)], axis=0)
                    second = jnp.concatenate([planes[ph, sh, q + 1, kt] for q in range(4)], axis=0)
                    k0, k1, k2 = (wf[kt, kh, kw] for kw in range(3))
                    if b == 0:
                        cols += [first, second[:, 128:]]
                        rhs += [k1, k0, zero, k2]
                    else:
                        cols += [first[:, :256], second]
                        rhs += [k0, zero, k2, k1]
            d = dot(jnp.concatenate(cols, axis=1), jnp.concatenate(rhs, axis=0))
            for q in range(4):
                l = jnp.concatenate([dense(lift.at[a, q + b, b + c], a, 2) for c in range(2)], axis=1)
                v = d[48 * q:48 * q + 48] + ((l[:, 64:] if b else l[:, :c1]) + b2)
                back[a, 0, pl.ds(2 * q + b, 48, stride=8), :] = v[:, :128]
                back[a, 1, pl.ds(2 * q + b, 48, stride=8), 0:64] = v[:, 128:]
        for t in range(4):
            for i in range(12):
                at = 96 * t + 8 * i
                out[t, 2 * i + a] = jnp.concatenate([back[a, 0, at:at + 8, :], back[a, 1, at:at + 8, 0:64]], axis=1).astype(BF)


def block(x, gain0, wc, bias0, wu, bias1, gain1, wf, bias2, *, nt, ns):
    c0, c1 = wc.shape[-1], wf.shape[-1]
    at = lambda t, s: t * ns + s
    vm = pl.BlockSpec(memory_space=pltpu.VMEM)
    hbm = pl.BlockSpec(memory_space=pltpu.HBM)
    far = lambda v: pltpu.with_memory_space_constraint(v, pltpu.HBM)
    two = lambda v: v.reshape(1, -1)
    axes = ("tm", "strip")
    prev = lax.ppermute(x, axes, [(at(t, s), at(t + 1, s)) for t in range(nt - 1) for s in range(ns)])
    w4, wv, part, mine = pl.pallas_call(
        own,
        out_shape=(jax.ShapeDtypeStruct((4 * c0, 4 * c1), BF), jax.ShapeDtypeStruct(wc.shape, BF),
                   jax.ShapeDtypeStruct((256, c0), F32), jax.ShapeDtypeStruct((2, 4, 2) + x.shape[2:], BF)),
        in_specs=[hbm] * 4,
        out_specs=(vm, vm, vm, vm),
        scratch_shapes=[
            pltpu.VMEM(x.shape, BF),
            pltpu.VMEM((c0,), F32),
            pltpu.VMEM((3, 3, c1, c0), BF),
            pltpu.VMEM((4 * c1, 4 * c0), BF),
            pltpu.VMEM((3, 272, 128), F32),
            pltpu.VMEM((3, 256, c0), BF),
            pltpu.SemaphoreType.DMA((6,)),
        ],
        compiler_params=pltpu.CompilerParams(vmem_limit_bytes=26 << 20),
    )(far(x), far(gain0), far(wc), far(jnp.swapaxes(wu, 2, 3)))
    mid = jax.ShapeDtypeStruct((384, c0), F32)
    left = jax.ShapeDtypeStruct((3, 256, c0), BF)
    rows = jax.ShapeDtypeStruct((8, 2) + x.shape[2:], BF)
    params = pltpu.CompilerParams(vmem_limit_bytes=14 << 20)
    to_inner, to_outer, sums, laid = pl.pallas_call(
        early,
        out_shape=(rows, rows, mid, left),
        in_specs=[vm] * 6,
        out_specs=(vm,) * 4,
        scratch_shapes=[pltpu.VMEM((3, 272, 128), F32)],
        compiler_params=params,
    )(part, prev, mine, gain0, wv, bias0)
    inner = lax.ppermute(to_inner, axes, [(at(t, s), at(t, s ^ 1)) for t in range(nt) for s in range(ns)])
    outer = lax.ppermute(to_outer, axes,
                         [(at(t, s), at(t, s + 1 if s % 2 else s - 1)) for t in range(nt) for s in range(1, ns - 1)])
    sums, _ = pl.pallas_call(
        old,
        out_shape=(mid, left),
        in_specs=[vm] * 7,
        out_specs=(vm, vm),
        scratch_shapes=[pltpu.VMEM((3, 272, 128), F32)],
        input_output_aliases={5: 0, 6: 1},
        compiler_params=params,
    )(part, prev, gain0, wv, bias0, sums, laid)
    return pl.pallas_call(
        functools.partial(kernel, ns - 1),
        out_shape=jax.ShapeDtypeStruct((4, 24, 8, c1), BF),
        in_specs=[vm] * 10,
        out_specs=vm,
        scratch_shapes=[
            pltpu.VMEM((3, 128, 128), F32),
            pltpu.VMEM((2, 384, c0), BF),
            pltpu.VMEM((3, 3, 128, c0), BF),
            pltpu.VMEM((3, 128, 128), F32),
            pltpu.VMEM((3, 400, 128), F32),
            pltpu.VMEM((2, 5, 3, 112, 128), F32),
            pltpu.VMEM((2, 5, 3, 112, 128), F32),
            pltpu.VMEM((2, 2, 5, 3, 48, 2 * c1), BF),
            pltpu.VMEM((2, 2, 384, 128), F32),
        ],
        compiler_params=pltpu.CompilerParams(vmem_limit_bytes=14 << 20),
    )(sums, inner, outer, gain0, wv, w4, two(bias1), two(gain1), wf, two(bias2))


def solution(mesh):
    nt, ns = mesh.shape["tm"], mesh.shape["strip"]
    part = P("tm", "strip", None, None)
    return jax.shard_map(
        functools.partial(block, nt=nt, ns=ns), mesh=mesh,
        in_specs=(part,) + (P(),) * 8, out_specs=part, check_vma=False)
```

```python
import functools

import jax
import jax.numpy as jnp
from jax import lax
from jax.experimental import pallas as pl
from jax.experimental.pallas import tpu as pltpu
from jax.sharding import PartitionSpec as P


EPS = 1e-6
BF = jnp.bfloat16
F32 = jnp.float32


def silu(v):
    half = 0.5 * v
    return half + half * jnp.tanh(half)


def dot(a, b):
    return jnp.dot(a, b, preferred_element_type=F32)


def phases(wu, w4, turned):
    c1, c0 = wu.shape[2:]
    for r in range(0, c1, 16):
        f = [[wu[kh, kw, r:r + 16, :].astype(F32) for kw in range(3)] for kh in range(3)]
        cols = [[(k[0], k[1] + k[2]), (k[0] + k[1], k[2])] for k in f]
        for wcol in range(2):
            tap = [[cols[kh][b][wcol] for b in range(2)] for kh in range(3)]
            first = tap[0] + [tap[0][b] + tap[1][b] for b in range(2)]
            second = [tap[1][b] + tap[2][b] for b in range(2)] + tap[2]
            for hrow, parts in enumerate((first, second)):
                at = (2 * wcol + hrow) * c0
                for i, v in enumerate(parts):
                    turned[c1 * i + r:c1 * i + r + 16, at:at + c0] = v.astype(BF)
    for k in range(0, 4 * c0, 128):
        w4[k:k + 128, :] = turned[:, k:k + 128].T


def put(raw, row, v):
    for c in range(3):
        raw[c, row:row + v.shape[0], :] = v[:, 128 * c:128 * c + 128]


def normed(raw, row, g0):
    v = jnp.concatenate([raw[c, row:row + 64, :] for c in range(3)], axis=1)
    r = lax.rsqrt(jnp.mean(v * v, axis=-1, keepdims=True) + EPS)
    return silu(v * r * g0)


def spread(raw, left, t):
    for kh in range(3):
        for w in range(4):
            for c in range(3):
                v = raw[c, pl.ds(64 * t + 4 * kh + w, 16, stride=4), :]
                left[kh, 64 * t + 16 * w:64 * t + 16 * w + 16, 128 * c:128 * c + 128] = v.astype(BF)


SPAN = ((0, 3), (0, 4), (1, 3))


def blank(raw, n):
    zero = jnp.zeros((8, 3 * raw.shape[-1]), F32)
    for t in range(n):
        put(raw, 64 * t, zero)
        put(raw, 64 * t + 56, zero)
    put(raw, 64 * n, zero)


def gather(left, lo, m, first, n):
    return jnp.concatenate(
        [jnp.concatenate([left[kh, 64 * t + 16 * lo:64 * t + 16 * (lo + m), :] for t in range(first, first + n)], axis=0)
         for kh in range(3)], axis=1)


def stack(wc, kt, kw):
    return jnp.concatenate([wc[kt, kh, kw] for kh in range(3)], axis=0)


def own(x_hbm, gain0_hbm, wc, wu_hbm, w4, wv, part, mine, x, gain0, wu, turned, raw, left, sems):
    c0 = x.shape[-1]
    get_x = pltpu.make_async_copy(x_hbm, x, sems.at[3])
    get_x.start()
    get_g = pltpu.make_async_copy(gain0_hbm, gain0, sems.at[5])
    get_g.start()
    get_u = pltpu.make_async_copy(wu_hbm, wu, sems.at[4])
    get_u.start()
    copies = {}
    for kt in (2, 1, 0):
        copies[kt] = pltpu.make_async_copy(wc.at[kt], wv.at[kt], sems.at[kt])
        copies[kt].start()
    blank(raw, 4)
    get_x.wait()
    mine[0] = x[:, :2]
    mine[1] = x[:, 10:]
    get_g.wait()
    g0 = gain0[...].reshape(1, c0)
    for t in range(4):
        for h in range(12):
            put(raw, 64 * t + 8 + 4 * h, x[t, h].astype(F32))
        put(raw, 64 * t, normed(raw, 64 * t, g0))
    for t in range(4):
        spread(raw, left, t)
    get_u.wait()
    phases(wu, w4, turned)
    for kt in (2, 1, 0):
        copies[kt].wait()
        n = kt + 2
        for kw in (1, 0, 2):
            lo, m = SPAN[kw]
            d = dot(gather(left, lo, m, 0, n), stack(wv, kt, kw))
            for t in range(n):
                at = 64 * (t + 2 - kt) + 16 * (lo + 1 - kw)
                v = d[16 * m * t:16 * m * (t + 1)]
                if kt == 2 and kw == 1:
                    part[at:at + 16 * m, :] = v
                else:
                    part[at:at + 16 * m, :] += v


def shares(wc, mid, left, kts):
    for kt in kts:
        n = 4 - kt
        for kw in range(3):
            lo, m = SPAN[kw]
            d = dot(gather(left, lo, m, kt, n), stack(wc, kt, kw))
            for u in range(n):
                at = 64 * u + 16 * (lo + 1 - kw)
                mid[at:at + 16 * m, :] += d[16 * m * u:16 * m * (u + 1)]


def begin(part, prev, gain0, wc, bias0, mid, left, raw):
    c0 = prev.shape[-1]
    g0 = gain0[...].reshape(1, c0)
    b0 = bias0[...].reshape(1, c0)
    blank(raw, 4)
    for t in range(4):
        for h in range(12):
            put(raw, 64 * t + 8 + 4 * h, prev[t, h].astype(F32))
        put(raw, 64 * t, normed(raw, 64 * t, g0))
    for t in range(4):
        spread(raw, left, t)
    mid[0:128, :] = jnp.broadcast_to(b0, (128, c0))
    mid[128:384, :] = part[...] + b0
    shares(wc, mid, left, (0,))


def early(part, prev, mine, gain0, wc, bias0, inner, outer, mid, left, raw):
    odd = lax.axis_index("strip") % 2 == 1

    @pl.when(odd)
    def _():
        inner[0:4], inner[4:8] = prev[:, :2], mine[0]
        outer[0:4], outer[4:8] = prev[:, 10:], mine[1]
        begin(part, prev, gain0, wc, bias0, mid, left, raw)

    @pl.when(jnp.logical_not(odd))
    def _():
        inner[0:4], inner[4:8] = prev[:, 10:], mine[1]
        outer[0:4], outer[4:8] = prev[:, :2], mine[0]


def old(part, prev, gain0, wc, bias0, mid_in, left_in, mid, left, raw):
    @pl.when(lax.axis_index("strip") % 2 == 0)
    def _():
        begin(part, prev, gain0, wc, bias0, mid, left, raw)

    shares(wc, mid, left, (1, 2))


def kernel(last, sums, inner, outer, gain0, wc, w4, bias1, gain1, wf, bias2, out,
           raw, left, ends, tail, mid, lift, lines, planes, back):
    group = lax.axis_index("tm")
    strip = lax.axis_index("strip")
    c0 = wc.shape[-1]
    c1 = wf.shape[-1]
    odd = strip % 2 == 1

    sub = lax.broadcasted_iota(jnp.int32, (8, 128), 0)

    @pl.when(strip >= 0)
    def _():
        for t in range(8):
            for i in range(2):
                a, b = inner[t, i].astype(F32), outer[t, i].astype(F32)
                put(raw, 16 * t + 4 * i, jnp.where(odd, a, b))
                put(raw, 16 * t + 8 + 4 * i, jnp.where(odd, b, a))
        g0 = gain0[...].reshape(1, c0)
        row = lax.broadcasted_iota(jnp.int32, (8, c0), 0)
        none = jnp.zeros((8, c0), F32)
        for half in range(2):
            v = normed(raw, 64 * half, g0)
            for i in range(4):
                t = 4 * half + i
                up, down = v[16 * i:16 * i + 8], v[16 * i + 8:16 * i + 16]
                for kh in range(3):
                    a = (up, jnp.where(row < 4, pltpu.roll(up, 4, 0), 0.0), none)[kh]
                    b = (none, jnp.where(row < 4, 0.0, pltpu.roll(down, 4, 0)), down)[kh]
                    for kw in range(3):
                        if kw == 0:
                            e = [jnp.where(row % 4 == 0, 0.0, pltpu.roll(z, 1, 0)) for z in (a, b)]
                        elif kw == 2:
                            e = [jnp.where(row % 4 == 3, 0.0, pltpu.roll(z, 7, 0)) for z in (a, b)]
                        else:
                            e = [a, b]
                        ends[kw, kh, 16 * t:16 * t + 16, :] = jnp.concatenate(e, axis=0).astype(BF)
        every = [(kt, kw, kh) for kt in range(3) for kw in range(3) for kh in range(3)]
        d = dot(jnp.concatenate([ends[kw, kh, 16 * kt:16 * kt + 96, :] for kt, kw, kh in every], axis=1),
                jnp.concatenate([wc[kt, kh, kw] for kt, kw, kh in every], axis=0))
        for c in range(3):
            tail[c, 8:104, :] = d[:, 128 * c:128 * c + 128]
        keep_top = jnp.logical_or(strip > 0, sub != 0)
        keep_end = jnp.logical_or(strip < last, sub != 5)
        for t in range(6):
            for w in range(4):
                at = 64 * t + 16 * w
                for c in range(3):
                    lanes = slice(128 * c, 128 * c + 128)
                    top = sums[at:at + 8, lanes] + jnp.where(sub < 2, tail[c, pl.ds(16 * t + w + 8, 8, stride=4), :], 0.0)
                    add = jnp.where(sub // 2 == 2, tail[c, pl.ds(16 * t + w, 8, stride=4), :], 0.0)
                    end = sums[at + 8:at + 16, lanes] + add
                    v = jnp.concatenate([jnp.where(keep_top, top, 0.0), jnp.where(keep_end, end, 0.0)], axis=0)
                    mid[c, at:at + 16, :] = v
                    left[0, at:at + 16, lanes] = v.astype(BF)
        for at in range(0, 384, 16):
            for c in range(3):
                left[1, at:at + 16, 128 * c:128 * c + 128] = mid[c, at + 1:at + 17, :].astype(BF)

    def ups(lo, n, first, count):
        both = [jnp.concatenate([left[i, 64 * t + 16 * lo:64 * t + 16 * (lo + n), :] for t in range(first, first + count)],
                                axis=0) for i in range(2)]
        return jnp.concatenate(both, axis=1)

    def thirds(v):
        v = jnp.concatenate([v, v], axis=1)
        return [v[:, 128 * c:128 * c + 128] for c in range(3)]

    b1 = thirds(bias1[...])
    g1 = thirds(0.5 * gain1[...])
    low = lax.broadcasted_iota(jnp.int32, (16, 128), 1) < 64
    row = lax.broadcasted_iota(jnp.int32, (16, 1), 0)
    ok_end = jnp.logical_or(strip < last, row != 12)
    ok_top = jnp.logical_or(strip > 0, row != 0)
    early = [jnp.logical_and(ok, group > 0) for ok in (ok_end, ok_top)]

    def finish(u, p, t, a):
        l = [None if u[c] is None else (u[c] + b1[c]).astype(BF).astype(F32) for c in range(3)]
        at = 16 * t
        for c in range(3):
            if l[c] is not None:
                lift[a, p, c, at:at + 16, :] = l[c]
        ok = early[a] if t < 2 else (ok_end, ok_top)[a]
        mids = l[1] * l[1]
        part = jnp.where(low, mids, 0.0)
        re = ro = jnp.zeros((16, 1), F32)
        if p < 4:
            re = jnp.sum(l[0] * l[0] + part, axis=-1, keepdims=True) * (1.0 / c1)
            re = jnp.where(ok, lax.rsqrt(re + EPS), 0.0)
        if p > 0:
            ro = jnp.sum(l[2] * l[2] + (mids - part), axis=-1, keepdims=True) * (1.0 / c1)
            ro = jnp.where(ok, lax.rsqrt(ro + EPS), 0.0)
        for c, r in enumerate((re, jnp.where(low, re, ro), ro)):
            if l[c] is not None:
                h = l[c] * (r * g1[c])
                lines[a, p, c, at:at + 16, :] = h + h * jnp.tanh(h)

    def dense(ref, s, kt):
        rows = lambda t, k: ref[16 * t + s + k:16 * t + s + k + 8, :]
        seam = lambda t: jnp.where(sub < 4, rows(t, 8), rows(t + 1, -4))
        return jnp.concatenate(
            [rows(kt, 0), seam(kt), rows(kt + 1, 4), rows(kt + 2, 0), seam(kt + 2), rows(kt + 3, 4)], axis=0)

    def pack(p, kts=range(3)):
        for kt in kts:
            for a in range(2):
                for s in range(2):
                    for c in range(3):
                        none = p == 0 and c == 2 or p == 4 and c == 0
                        v = jnp.zeros((48, 128), BF) if none else dense(lines.at[a, p, c], s, kt).astype(BF)
                        planes[a, s, p, kt, :, 128 * c:128 * c + 128] = v

    def edge(p):
        lhs, rhs = (ups(0, 1, 0, 6), slice(2 * c0, 4 * c0)) if p == 0 else (ups(3, 1, 0, 6), slice(0, 2 * c0))
        u = []
        for a in range(2):
            n = 2 * c1 * a + (0 if p == 0 else 128)
            d = dot(lhs, w4[rhs, n:n + 256])
            u.append([d[:, :128], d[:, 128:], None] if p == 0 else [None, d[:, :128], d[:, 128:]])
        return u

    def chunk(first, count):
        return dot(jnp.concatenate([ups(0, 3, first, count), ups(1, 3, first, count)], axis=1), w4[...])

    def finish_edge(u, p):
        for t in range(6):
            for a in range(2):
                finish([v if v is None else v[16 * t:16 * t + 16] for v in u[a]], p, t, a)
        pack(p)

    def finish_chunk(u, first, count):
        for t in range(count):
            for p in range(1, 4):
                at = 48 * t + 16 * (p - 1)
                for a in range(2):
                    n = 2 * c1 * a
                    finish([u[at:at + 16, n + 128 * c:n + 128 * c + 128] for c in range(3)], p, first + t, a)

    ua = chunk(0, 4)
    u0, u4 = edge(0), edge(4)
    finish_chunk(ua, 0, 4)
    ub = chunk(4, 2)
    for p in range(1, 4):
        pack(p, (0,))
    finish_edge(u0, 0)
    finish_edge(u4, 4)
    finish_chunk(ub, 4, 2)
    for p in range(1, 4):
        pack(p, (1, 2))
    b2 = bias2[...]
    zero = jnp.zeros((64, c1), BF)
    for a in range(2):
        reads = ((1, 0), (0, 0), (1, 1)) if a == 0 else ((0, 0), (1, 1), (0, 1))
        for b in (1, 0):
            cols, rhs = [], []
            for kt in range(3):
                for kh in range(3):
                    ph, sh = reads[kh]
                    first = jnp.concatenate([planes[ph, sh, q, kt] for q in range(4)], axis=0)
                    second = jnp.concatenate([planes[ph, sh, q + 1, kt] for q in range(4)], axis=0)
                    k0, k1, k2 = (wf[kt, kh, kw] for kw in range(3))
                    if b == 0:
                        cols += [first, second[:, 128:]]
                        rhs += [k1, k0, zero, k2]
                    else:
                        cols += [first[:, :256], second]
                        rhs += [k0, zero, k2, k1]
            d = dot(jnp.concatenate(cols, axis=1), jnp.concatenate(rhs, axis=0))
            for q in range(4):
                l = jnp.concatenate([dense(lift.at[a, q + b, b + c], a, 2) for c in range(2)], axis=1)
                v = d[48 * q:48 * q + 48] + ((l[:, 64:] if b else l[:, :c1]) + b2)
                back[a, 0, pl.ds(2 * q + b, 48, stride=8), :] = v[:, :128]
                back[a, 1, pl.ds(2 * q + b, 48, stride=8), 0:64] = v[:, 128:]
        for t in range(4):
            for i in range(12):
                at = 96 * t + 8 * i
                out[t, 2 * i + a] = jnp.concatenate([back[a, 0, at:at + 8, :], back[a, 1, at:at + 8, 0:64]], axis=1).astype(BF)


def block(x, gain0, wc, bias0, wu, bias1, gain1, wf, bias2, *, nt, ns):
    c0, c1 = wc.shape[-1], wf.shape[-1]
    at = lambda t, s: t * ns + s
    vm = pl.BlockSpec(memory_space=pltpu.VMEM)
    hbm = pl.BlockSpec(memory_space=pltpu.HBM)
    far = lambda v: pltpu.with_memory_space_constraint(v, pltpu.HBM)
    two = lambda v: v.reshape(1, -1)
    axes = ("tm", "strip")
    prev = lax.ppermute(x, axes, [(at(t, s), at(t + 1, s)) for t in range(nt - 1) for s in range(ns)])
    w4, wv, part, mine = pl.pallas_call(
        own,
        out_shape=(jax.ShapeDtypeStruct((4 * c0, 4 * c1), BF), jax.ShapeDtypeStruct(wc.shape, BF),
                   jax.ShapeDtypeStruct((256, c0), F32), jax.ShapeDtypeStruct((2, 4, 2) + x.shape[2:], BF)),
        in_specs=[hbm] * 4,
        out_specs=(vm, vm, vm, vm),
        scratch_shapes=[
            pltpu.VMEM(x.shape, BF),
            pltpu.VMEM((c0,), F32),
            pltpu.VMEM((3, 3, c1, c0), BF),
            pltpu.VMEM((4 * c1, 4 * c0), BF),
            pltpu.VMEM((3, 272, 128), F32),
            pltpu.VMEM((3, 256, c0), BF),
            pltpu.SemaphoreType.DMA((6,)),
        ],
        compiler_params=pltpu.CompilerParams(vmem_limit_bytes=26 << 20),
    )(far(x), far(gain0), far(wc), far(jnp.swapaxes(wu, 2, 3)))
    mid = jax.ShapeDtypeStruct((384, c0), F32)
    left = jax.ShapeDtypeStruct((3, 256, c0), BF)
    rows = jax.ShapeDtypeStruct((8, 2) + x.shape[2:], BF)
    params = pltpu.CompilerParams(vmem_limit_bytes=14 << 20)
    to_inner, to_outer, sums, laid = pl.pallas_call(
        early,
        out_shape=(rows, rows, mid, left),
        in_specs=[vm] * 6,
        out_specs=(vm,) * 4,
        scratch_shapes=[pltpu.VMEM((3, 272, 128), F32)],
        compiler_params=params,
    )(part, prev, mine, gain0, wv, bias0)
    inner = lax.ppermute(to_inner, axes, [(at(t, s), at(t, s ^ 1)) for t in range(nt) for s in range(ns)])
    outer = lax.ppermute(to_outer, axes,
                         [(at(t, s), at(t, s + 1 if s % 2 else s - 1)) for t in range(nt) for s in range(1, ns - 1)])
    sums, _ = pl.pallas_call(
        old,
        out_shape=(mid, left),
        in_specs=[vm] * 7,
        out_specs=(vm, vm),
        scratch_shapes=[pltpu.VMEM((3, 272, 128), F32)],
        input_output_aliases={5: 0, 6: 1},
        compiler_params=params,
    )(part, prev, gain0, wv, bias0, sums, laid)
    return pl.pallas_call(
        functools.partial(kernel, ns - 1),
        out_shape=jax.ShapeDtypeStruct((4, 24, 8, c1), BF),
        in_specs=[vm] * 10,
        out_specs=vm,
        scratch_shapes=[
            pltpu.VMEM((3, 128, 128), F32),
            pltpu.VMEM((2, 384, c0), BF),
            pltpu.VMEM((3, 3, 128, c0), BF),
            pltpu.VMEM((3, 128, 128), F32),
            pltpu.VMEM((3, 400, 128), F32),
            pltpu.VMEM((2, 5, 3, 112, 128), F32),
            pltpu.VMEM((2, 5, 3, 112, 128), F32),
            pltpu.VMEM((2, 2, 5, 3, 48, 2 * c1), BF),
            pltpu.VMEM((2, 2, 384, 128), F32),
        ],
        compiler_params=pltpu.CompilerParams(vmem_limit_bytes=14 << 20),
    )(sums, inner, outer, gain0, wv, w4, two(bias1), two(gain1), wf, two(bias2))


def solution(mesh):
    nt, ns = mesh.shape["tm"], mesh.shape["strip"]
    part = P("tm", "strip", None, None)
    return jax.shard_map(
        functools.partial(block, nt=nt, ns=ns), mesh=mesh,
        in_specs=(part,) + (P(),) * 8, out_specs=part, check_vma=False)
```

```python
import functools

import jax
import jax.numpy as jnp
from jax import lax
from jax.experimental import pallas as pl
from jax.experimental.pallas import tpu as pltpu
from jax.sharding import PartitionSpec as P


EPS = 1e-6
BF = jnp.bfloat16
F32 = jnp.float32


def silu(v):
    half = 0.5 * v
    return half + half * jnp.tanh(half)


def dot(a, b):
    return jnp.dot(a, b, preferred_element_type=F32)


def phases(wu, w4, turned):
    c1, c0 = wu.shape[2:]
    for r in range(0, c1, 16):
        f = [[wu[kh, kw, r:r + 16, :].astype(F32) for kw in range(3)] for kh in range(3)]
        cols = [[(k[0], k[1] + k[2]), (k[0] + k[1], k[2])] for k in f]
        for wcol in range(2):
            tap = [[cols[kh][b][wcol] for b in range(2)] for kh in range(3)]
            first = tap[0] + [tap[0][b] + tap[1][b] for b in range(2)]
            second = [tap[1][b] + tap[2][b] for b in range(2)] + tap[2]
            for hrow, parts in enumerate((first, second)):
                at = (2 * wcol + hrow) * c0
                for i, v in enumerate(parts):
                    turned[c1 * i + r:c1 * i + r + 16, at:at + c0] = v.astype(BF)
    for k in range(0, 4 * c0, 128):
        w4[k:k + 128, :] = turned[:, k:k + 128].T


def put(raw, row, v):
    for c in range(3):
        raw[c, row:row + v.shape[0], :] = v[:, 128 * c:128 * c + 128]


def normed(raw, row, g0):
    v = jnp.concatenate([raw[c, row:row + 64, :] for c in range(3)], axis=1)
    r = lax.rsqrt(jnp.mean(v * v, axis=-1, keepdims=True) + EPS)
    return silu(v * r * g0)


def spread(raw, left, t):
    for kh in range(3):
        for w in range(4):
            for c in range(3):
                v = raw[c, pl.ds(64 * t + 4 * kh + w, 16, stride=4), :]
                left[kh, 64 * t + 16 * w:64 * t + 16 * w + 16, 128 * c:128 * c + 128] = v.astype(BF)


SPAN = ((0, 3), (0, 4), (1, 3))


def blank(raw, n):
    zero = jnp.zeros((8, 3 * raw.shape[-1]), F32)
    for t in range(n):
        put(raw, 64 * t, zero)
        put(raw, 64 * t + 56, zero)
    put(raw, 64 * n, zero)


def gather(left, lo, m, first, n):
    return jnp.concatenate(
        [jnp.concatenate([left[kh, 64 * t + 16 * lo:64 * t + 16 * (lo + m), :] for t in range(first, first + n)], axis=0)
         for kh in range(3)], axis=1)


def stack(wc, kt, kw):
    return jnp.concatenate([wc[kt, kh, kw] for kh in range(3)], axis=0)


def own(x_hbm, gain0_hbm, wc, wu_hbm, w4, wv, part, mine, x, gain0, wu, turned, raw, left, sems):
    c0 = x.shape[-1]
    get_x = pltpu.make_async_copy(x_hbm, x, sems.at[3])
    get_x.start()
    get_g = pltpu.make_async_copy(gain0_hbm, gain0, sems.at[5])
    get_g.start()
    get_u = pltpu.make_async_copy(wu_hbm, wu, sems.at[4])
    get_u.start()
    copies = {}
    for kt in (2, 1, 0):
        copies[kt] = pltpu.make_async_copy(wc.at[kt], wv.at[kt], sems.at[kt])
        copies[kt].start()
    blank(raw, 4)
    get_x.wait()
    mine[0] = x[:, :2]
    mine[1] = x[:, 10:]
    get_g.wait()
    g0 = gain0[...].reshape(1, c0)
    for t in range(4):
        for h in range(12):
            put(raw, 64 * t + 8 + 4 * h, x[t, h].astype(F32))
        put(raw, 64 * t, normed(raw, 64 * t, g0))
    for t in range(4):
        spread(raw, left, t)
    get_u.wait()
    phases(wu, w4, turned)
    for kt in (2, 1, 0):
        copies[kt].wait()
        n = kt + 2
        for kw in (1, 0, 2):
            lo, m = SPAN[kw]
            d = dot(gather(left, lo, m, 0, n), stack(wv, kt, kw))
            for t in range(n):
                at = 64 * (t + 2 - kt) + 16 * (lo + 1 - kw)
                v = d[16 * m * t:16 * m * (t + 1)]
                if kt == 2 and kw == 1:
                    part[at:at + 16 * m, :] = v
                else:
                    part[at:at + 16 * m, :] += v


def shares(wc, mid, left, kts):
    for kt in kts:
        n = 4 - kt
        for kw in range(3):
            lo, m = SPAN[kw]
            d = dot(gather(left, lo, m, kt, n), stack(wc, kt, kw))
            for u in range(n):
                at = 64 * u + 16 * (lo + 1 - kw)
                mid[at:at + 16 * m, :] += d[16 * m * u:16 * m * (u + 1)]


def begin(part, prev, gain0, wc, bias0, mid, left, raw):
    c0 = prev.shape[-1]
    g0 = gain0[...].reshape(1, c0)
    b0 = bias0[...].reshape(1, c0)
    blank(raw, 4)
    for t in range(4):
        for h in range(12):
            put(raw, 64 * t + 8 + 4 * h, prev[t, h].astype(F32))
        put(raw, 64 * t, normed(raw, 64 * t, g0))
    for t in range(4):
        spread(raw, left, t)
    mid[0:128, :] = jnp.broadcast_to(b0, (128, c0))
    mid[128:384, :] = part[...] + b0
    shares(wc, mid, left, (0,))


def early(prev, mine, inner, outer):
    odd = lax.axis_index("strip") % 2 == 1

    @pl.when(odd)
    def _():
        inner[0:4], inner[4:8] = prev[:, :2], mine[0]
        outer[0:4], outer[4:8] = prev[:, 10:], mine[1]

    @pl.when(jnp.logical_not(odd))
    def _():
        inner[0:4], inner[4:8] = prev[:, 10:], mine[1]
        outer[0:4], outer[4:8] = prev[:, :2], mine[0]


def old(part, prev, gain0, wc, bias0, mid, left, raw):
    begin(part, prev, gain0, wc, bias0, mid, left, raw)
    shares(wc, mid, left, (1, 2))


def kernel(last, sums, inner, outer, gain0, wc, w4, bias1, gain1, wf, bias2, out,
           raw, left, ends, tail, mid, lift, lines, planes, back):
    group = lax.axis_index("tm")
    strip = lax.axis_index("strip")
    c0 = wc.shape[-1]
    c1 = wf.shape[-1]
    odd = strip % 2 == 1

    sub = lax.broadcasted_iota(jnp.int32, (8, 128), 0)

    @pl.when(strip >= 0)
    def _():
        for t in range(8):
            for i in range(2):
                a, b = inner[t, i].astype(F32), outer[t, i].astype(F32)
                put(raw, 16 * t + 4 * i, jnp.where(odd, a, b))
                put(raw, 16 * t + 8 + 4 * i, jnp.where(odd, b, a))
        g0 = gain0[...].reshape(1, c0)
        row = lax.broadcasted_iota(jnp.int32, (8, c0), 0)
        none = jnp.zeros((8, c0), F32)
        for half in range(2):
            v = normed(raw, 64 * half, g0)
            for i in range(4):
                t = 4 * half + i
                up, down = v[16 * i:16 * i + 8], v[16 * i + 8:16 * i + 16]
                for kh in range(3):
                    a = (up, jnp.where(row < 4, pltpu.roll(up, 4, 0), 0.0), none)[kh]
                    b = (none, jnp.where(row < 4, 0.0, pltpu.roll(down, 4, 0)), down)[kh]
                    for kw in range(3):
                        if kw == 0:
                            e = [jnp.where(row % 4 == 0, 0.0, pltpu.roll(z, 1, 0)) for z in (a, b)]
                        elif kw == 2:
                            e = [jnp.where(row % 4 == 3, 0.0, pltpu.roll(z, 7, 0)) for z in (a, b)]
                        else:
                            e = [a, b]
                        ends[kw, kh, 16 * t:16 * t + 16, :] = jnp.concatenate(e, axis=0).astype(BF)
        every = [(kt, kw, kh) for kt in range(3) for kw in range(3) for kh in range(3)]
        d = dot(jnp.concatenate([ends[kw, kh, 16 * kt:16 * kt + 96, :] for kt, kw, kh in every], axis=1),
                jnp.concatenate([wc[kt, kh, kw] for kt, kw, kh in every], axis=0))
        for c in range(3):
            tail[c, 8:104, :] = d[:, 128 * c:128 * c + 128]
        keep_top = jnp.logical_or(strip > 0, sub != 0)
        keep_end = jnp.logical_or(strip < last, sub != 5)
        for t in range(6):
            for w in range(4):
                at = 64 * t + 16 * w
                for c in range(3):
                    lanes = slice(128 * c, 128 * c + 128)
                    top = sums[at:at + 8, lanes] + jnp.where(sub < 2, tail[c, pl.ds(16 * t + w + 8, 8, stride=4), :], 0.0)
                    add = jnp.where(sub // 2 == 2, tail[c, pl.ds(16 * t + w, 8, stride=4), :], 0.0)
                    end = sums[at + 8:at + 16, lanes] + add
                    v = jnp.concatenate([jnp.where(keep_top, top, 0.0), jnp.where(keep_end, end, 0.0)], axis=0)
                    mid[c, at:at + 16, :] = v
                    left[0, at:at + 16, lanes] = v.astype(BF)
        for at in range(0, 384, 16):
            for c in range(3):
                left[1, at:at + 16, 128 * c:128 * c + 128] = mid[c, at + 1:at + 17, :].astype(BF)

    def ups(lo, n, first, count):
        both = [jnp.concatenate([left[i, 64 * t + 16 * lo:64 * t + 16 * (lo + n), :] for t in range(first, first + count)],
                                axis=0) for i in range(2)]
        return jnp.concatenate(both, axis=1)

    def thirds(v):
        v = jnp.concatenate([v, v], axis=1)
        return [v[:, 128 * c:128 * c + 128] for c in range(3)]

    b1 = thirds(bias1[...])
    g1 = thirds(0.5 * gain1[...])
    low = lax.broadcasted_iota(jnp.int32, (16, 128), 1) < 64
    row = lax.broadcasted_iota(jnp.int32, (16, 1), 0)
    ok_end = jnp.logical_or(strip < last, row != 12)
    ok_top = jnp.logical_or(strip > 0, row != 0)
    early = [jnp.logical_and(ok, group > 0) for ok in (ok_end, ok_top)]

    def finish(u, p, t, a):
        l = [None if u[c] is None else (u[c] + b1[c]).astype(BF).astype(F32) for c in range(3)]
        at = 16 * t
        for c in range(3):
            if l[c] is not None:
                lift[a, p, c, at:at + 16, :] = l[c]
        ok = early[a] if t < 2 else (ok_end, ok_top)[a]
        mids = l[1] * l[1]
        part = jnp.where(low, mids, 0.0)
        re = ro = jnp.zeros((16, 1), F32)
        if p < 4:
            re = jnp.sum(l[0] * l[0] + part, axis=-1, keepdims=True) * (1.0 / c1)
            re = jnp.where(ok, lax.rsqrt(re + EPS), 0.0)
        if p > 0:
            ro = jnp.sum(l[2] * l[2] + (mids - part), axis=-1, keepdims=True) * (1.0 / c1)
            ro = jnp.where(ok, lax.rsqrt(ro + EPS), 0.0)
        for c, r in enumerate((re, jnp.where(low, re, ro), ro)):
            if l[c] is not None:
                h = l[c] * (r * g1[c])
                lines[a, p, c, at:at + 16, :] = h + h * jnp.tanh(h)

    def dense(ref, s, kt):
        rows = lambda t, k: ref[16 * t + s + k:16 * t + s + k + 8, :]
        seam = lambda t: jnp.where(sub < 4, rows(t, 8), rows(t + 1, -4))
        return jnp.concatenate(
            [rows(kt, 0), seam(kt), rows(kt + 1, 4), rows(kt + 2, 0), seam(kt + 2), rows(kt + 3, 4)], axis=0)

    def pack(p, kts=range(3)):
        for kt in kts:
            for a in range(2):
                for s in range(2):
                    for c in range(3):
                        none = p == 0 and c == 2 or p == 4 and c == 0
                        v = jnp.zeros((48, 128), BF) if none else dense(lines.at[a, p, c], s, kt).astype(BF)
                        planes[a, s, p, kt, :, 128 * c:128 * c + 128] = v

    def edge(p):
        lhs, rhs = (ups(0, 1, 0, 6), slice(2 * c0, 4 * c0)) if p == 0 else (ups(3, 1, 0, 6), slice(0, 2 * c0))
        u = []
        for a in range(2):
            n = 2 * c1 * a + (0 if p == 0 else 128)
            d = dot(lhs, w4[rhs, n:n + 256])
            u.append([d[:, :128], d[:, 128:], None] if p == 0 else [None, d[:, :128], d[:, 128:]])
        return u

    def chunk(first, count):
        return dot(jnp.concatenate([ups(0, 3, first, count), ups(1, 3, first, count)], axis=1), w4[...])

    def finish_edge(u, p):
        for t in range(6):
            for a in range(2):
                finish([v if v is None else v[16 * t:16 * t + 16] for v in u[a]], p, t, a)
        pack(p)

    def finish_chunk(u, first, count):
        for t in range(count):
            for p in range(1, 4):
                at = 48 * t + 16 * (p - 1)
                for a in range(2):
                    n = 2 * c1 * a
                    finish([u[at:at + 16, n + 128 * c:n + 128 * c + 128] for c in range(3)], p, first + t, a)

    ua = chunk(0, 4)
    u0, u4 = edge(0), edge(4)
    finish_chunk(ua, 0, 4)
    ub = chunk(4, 2)
    for p in range(1, 4):
        pack(p, (0,))
    finish_edge(u0, 0)
    finish_edge(u4, 4)
    finish_chunk(ub, 4, 2)
    for p in range(1, 4):
        pack(p, (1, 2))
    b2 = bias2[...]
    zero = jnp.zeros((64, c1), BF)
    for a in range(2):
        reads = ((1, 0), (0, 0), (1, 1)) if a == 0 else ((0, 0), (1, 1), (0, 1))
        for b in (1, 0):
            cols, rhs = [], []
            for kt in range(3):
                for kh in range(3):
                    ph, sh = reads[kh]
                    first = jnp.concatenate([planes[ph, sh, q, kt] for q in range(4)], axis=0)
                    second = jnp.concatenate([planes[ph, sh, q + 1, kt] for q in range(4)], axis=0)
                    k0, k1, k2 = (wf[kt, kh, kw] for kw in range(3))
                    if b == 0:
                        cols += [first, second[:, 128:]]
                        rhs += [k1, k0, zero, k2]
                    else:
                        cols += [first[:, :256], second]
                        rhs += [k0, zero, k2, k1]
            d = dot(jnp.concatenate(cols, axis=1), jnp.concatenate(rhs, axis=0))
            for q in range(4):
                l = jnp.concatenate([dense(lift.at[a, q + b, b + c], a, 2) for c in range(2)], axis=1)
                v = d[48 * q:48 * q + 48] + ((l[:, 64:] if b else l[:, :c1]) + b2)
                back[a, 0, pl.ds(2 * q + b, 48, stride=8), :] = v[:, :128]
                back[a, 1, pl.ds(2 * q + b, 48, stride=8), 0:64] = v[:, 128:]
        for t in range(4):
            for i in range(12):
                at = 96 * t + 8 * i
                out[t, 2 * i + a] = jnp.concatenate([back[a, 0, at:at + 8, :], back[a, 1, at:at + 8, 0:64]], axis=1).astype(BF)


def block(x, gain0, wc, bias0, wu, bias1, gain1, wf, bias2, *, nt, ns):
    c0, c1 = wc.shape[-1], wf.shape[-1]
    at = lambda t, s: t * ns + s
    vm = pl.BlockSpec(memory_space=pltpu.VMEM)
    hbm = pl.BlockSpec(memory_space=pltpu.HBM)
    far = lambda v: pltpu.with_memory_space_constraint(v, pltpu.HBM)
    two = lambda v: v.reshape(1, -1)
    axes = ("tm", "strip")
    prev = lax.ppermute(x, axes, [(at(t, s), at(t + 1, s)) for t in range(nt - 1) for s in range(ns)])
    w4, wv, part, mine = pl.pallas_call(
        own,
        out_shape=(jax.ShapeDtypeStruct((4 * c0, 4 * c1), BF), jax.ShapeDtypeStruct(wc.shape, BF),
                   jax.ShapeDtypeStruct((256, c0), F32), jax.ShapeDtypeStruct((2, 4, 2) + x.shape[2:], BF)),
        in_specs=[hbm] * 4,
        out_specs=(vm, vm, vm, vm),
        scratch_shapes=[
            pltpu.VMEM(x.shape, BF),
            pltpu.VMEM((c0,), F32),
            pltpu.VMEM((3, 3, c1, c0), BF),
            pltpu.VMEM((4 * c1, 4 * c0), BF),
            pltpu.VMEM((3, 272, 128), F32),
            pltpu.VMEM((3, 256, c0), BF),
            pltpu.SemaphoreType.DMA((6,)),
        ],
        compiler_params=pltpu.CompilerParams(vmem_limit_bytes=26 << 20),
    )(far(x), far(gain0), far(wc), far(jnp.swapaxes(wu, 2, 3)))
    rows = jax.ShapeDtypeStruct((8, 2) + x.shape[2:], BF)
    params = pltpu.CompilerParams(vmem_limit_bytes=14 << 20)
    to_inner, to_outer = pl.pallas_call(
        early,
        out_shape=(rows, rows),
        in_specs=[vm] * 2,
        out_specs=(vm, vm),
        compiler_params=params,
    )(prev, mine)
    inner = lax.ppermute(to_inner, axes, [(at(t, s), at(t, s ^ 1)) for t in range(nt) for s in range(ns)])
    outer = lax.ppermute(to_outer, axes,
                         [(at(t, s), at(t, s + 1 if s % 2 else s - 1)) for t in range(nt) for s in range(1, ns - 1)])
    sums = pl.pallas_call(
        old,
        out_shape=jax.ShapeDtypeStruct((384, c0), F32),
        in_specs=[vm] * 5,
        out_specs=vm,
        scratch_shapes=[pltpu.VMEM((3, 256, c0), BF), pltpu.VMEM((3, 272, 128), F32)],
        compiler_params=params,
    )(part, prev, gain0, wv, bias0)
    return pl.pallas_call(
        functools.partial(kernel, ns - 1),
        out_shape=jax.ShapeDtypeStruct((4, 24, 8, c1), BF),
        in_specs=[vm] * 10,
        out_specs=vm,
        scratch_shapes=[
            pltpu.VMEM((3, 128, 128), F32),
            pltpu.VMEM((2, 384, c0), BF),
            pltpu.VMEM((3, 3, 128, c0), BF),
            pltpu.VMEM((3, 128, 128), F32),
            pltpu.VMEM((3, 400, 128), F32),
            pltpu.VMEM((2, 5, 3, 112, 128), F32),
            pltpu.VMEM((2, 5, 3, 112, 128), F32),
            pltpu.VMEM((2, 2, 5, 3, 48, 2 * c1), BF),
            pltpu.VMEM((2, 2, 384, 128), F32),
        ],
        compiler_params=pltpu.CompilerParams(vmem_limit_bytes=14 << 20),
    )(sums, inner, outer, gain0, wv, w4, two(bias1), two(gain1), wf, two(bias2))


def solution(mesh):
    nt, ns = mesh.shape["tm"], mesh.shape["strip"]
    part = P("tm", "strip", None, None)
    return jax.shard_map(
        functools.partial(block, nt=nt, ns=ns), mesh=mesh,
        in_specs=(part,) + (P(),) * 8, out_specs=part, check_vma=False)
```
